256 devices in a mesh: seq: 64 (over x_hi, y, z), tp: 4 (over x_lo, core).
Axes of the slice: x: 4 (x_hi: 2, x_lo: 2; x = x_hi * 2 + x_lo), y: 4, z: 8, core: 2. Of those that a mesh axis runs over, the one named last changes fastest.
Arguments:
- mixer_input: bfloat16 [8192, 8192], P('seq', 'tp'), may hold values from -6 to 6
- gate_input: bfloat16 [8192, 8192], P('seq', 'tp'), may hold values from -6 to 6
- input_matrix: bfloat16 [8192, 1024], P('seq', 'tp'), may hold values from -6 to 6
- output_matrix: bfloat16 [8192, 1024], P('seq', 'tp'), may hold values from -6 to 6
- step_raw: float32 [8192, 128], P('seq', 'tp'), may hold values from -3 to 3
- step_bias: float32 [128], P('tp'), may hold values from -1 to 0.5
- decay_rate: float32 [128], P('tp'), may hold values from 0.0001 to 0.05
- skip_weight: float32 [128], P('tp'), may hold values from 0.5 to 1.5
- conv_mixer: float32 [4, 8192], P(None, 'tp'), may hold values from -3 to 3
- conv_input: float32 [4, 1024], P(None, 'tp'), may hold values from -3 to 3
- conv_output: float32 [4, 1024], P(None, 'tp'), may hold values from -3 to 3
- norm_gain: float32 [8192], P('tp'), may hold values from 0.5 to 1.5
- queries: bfloat16 [8192, 8192], P('seq', 'tp'), may hold values from -5 to 5
- keys: bfloat16 [8192, 1024], P('seq', 'tp'), may hold values from -5 to 5
- values: bfloat16 [8192, 1024], P('seq', 'tp'), may hold values from -6 to 6
Outputs:
- mixer_out: bfloat16 [8192, 8192], P('seq', 'tp')
- attention_out: bfloat16 [8192, 8192], P('seq', 'tp')
The draws below stay inside these ranges and needn't reach their ends.
All inputs are finite; a program needn't handle non-finite values.
Results may differ from the reference program's by a relative error of at most 0.007.
Values may be sent and summed in bfloat16 or wider, within the bound.
A program may use at most 192 MiB of HBM per device.

```python
import math
import jax
import jax.numpy as jnp
from jax import lax

MH = 128
P_SIZE = 64
STATE = 128
GROUPS = 8
QH = 64
KVH = 8
HD = 128
CONV = 4
SCAN_BLOCK = 128
INNER = 8192
TOKENS = 8192


def draw_queries(key, part):
    drawn = jnp.clip(jax.random.normal(jax.random.fold_in(key, 1), (TOKENS, QH * HD), jnp.float32), -5.0, 5.0)
    return drawn.astype(jnp.bfloat16)


def draw_keys(key, part):
    drawn = jnp.clip(jax.random.normal(jax.random.fold_in(key, 2), (TOKENS, KVH * HD), jnp.float32), -5.0, 5.0)
    return drawn.astype(jnp.bfloat16)


def block_levels(stream_key, shape, cuts, least, top_value):
    factor_of = 1.0
    for dim, parts in cuts:
        draws = jax.random.uniform(jax.random.fold_in(jax.random.fold_in(stream_key, 6), dim), (parts,), jnp.float32, least / len(cuts), top_value / len(cuts))
        factor_of = factor_of * jnp.repeat(jnp.exp(draws), shape[dim] // parts).reshape((-1,) + (1,) * (len(shape) - 1 - dim))
    return factor_of


def normal_values(own_key, extent, width, bound, shards=(), held_as=jnp.bfloat16):
    values = width * jax.random.normal(own_key, extent, jnp.float32)
    if shards:
        values = values * block_levels(own_key, extent, shards, -0.22, 0.18)
    return jnp.clip(values, -bound, bound).astype(held_as)


def setup_inputs(seed: int = 0) -> dict:
    splits = jax.random.split(jax.random.key(seed), 16)
    mixer_input = normal_values(splits[0], (TOKENS, INNER), 1.0, 6.0, ((0, 64), (1, 4)))
    gate_input = normal_values(splits[1], (TOKENS, INNER), 1.0, 6.0, ((0, 64), (1, 4)))
    input_matrix = normal_values(splits[2], (TOKENS, GROUPS * STATE), 1.0, 6.0, ((0, 64), (1, 4)))
    output_matrix = normal_values(splits[3], (TOKENS, GROUPS * STATE), 1.0, 6.0, ((0, 64), (1, 4)))
    step_raw = normal_values(splits[4], (TOKENS, MH), 0.5, 3.0, ((0, 64), (1, 4)), jnp.float32)
    step_bias = jnp.clip(-1.0 + 1.5 * jax.random.uniform(splits[5], (MH,), jnp.float32) ** block_levels(splits[5], (MH,), ((0, 4),), -0.2, 0.2), -1.0, 0.5)
    decay_rate = jnp.clip(jnp.exp(math.log(0.05) - 6.214608 * jax.random.uniform(splits[6], (MH,), jnp.float32) ** block_levels(splits[6], (MH,), ((0, 4),), -0.2, 0.2)), 0.0001, 0.05)
    skip_weight = jnp.clip(0.5 + 1.0 * jax.random.uniform(splits[7], (MH,), jnp.float32) ** block_levels(splits[7], (MH,), ((0, 4),), -0.2, 0.2), 0.5, 1.5)
    conv_mixer = normal_values(splits[8], (CONV, INNER), CONV ** -0.5, 3.0, ((1, 4),), jnp.float32)
    conv_input = normal_values(splits[9], (CONV, GROUPS * STATE), CONV ** -0.5, 3.0, ((1, 4),), jnp.float32)
    conv_output = normal_values(splits[10], (CONV, GROUPS * STATE), CONV ** -0.5, 3.0, ((1, 4),), jnp.float32)
    norm_gain = jnp.clip(1.0 + 0.1 * jax.random.normal(splits[11], (INNER,), jnp.float32), 0.5, 1.5)
    queries = draw_queries(jax.random.fold_in(splits[15], 71), 0)
    keys = draw_keys(jax.random.fold_in(splits[15], 71), 0)
    values = normal_values(splits[14], (TOKENS, KVH * HD), 1.0, 6.0, ((0, 64), (1, 4)))
    return {"mixer_input": mixer_input, "gate_input": gate_input, "input_matrix": input_matrix, "output_matrix": output_matrix, "step_raw": step_raw, "step_bias": step_bias, "decay_rate": decay_rate, "skip_weight": skip_weight, "conv_mixer": conv_mixer, "conv_input": conv_input, "conv_output": conv_output, "norm_gain": norm_gain, "queries": queries, "keys": keys, "values": values}


HIGHEST = lax.Precision.HIGHEST
norm_epsilon = 1e-05
lowest_score = -1e+30

def conv_silu(raw_rows, weights, history):
    padded = jnp.concatenate([history, raw_rows], axis=0).astype(jnp.float32)
    length = raw_rows.shape[0]
    summed = jnp.zeros((length, raw_rows.shape[1]), jnp.float32)
    for offset in range(weights.shape[0]):
        summed = summed + weights[offset][None, :] * padded[offset:offset + length]
    return jax.nn.silu(summed)

def ssd_block(signal, b_state, c_state, step_size, rates, carried):
    group_heads = signal.shape[1] // b_state.shape[1]
    log_decay = jnp.cumsum(-step_size * rates[None, :], axis=0)
    length = signal.shape[0]
    places = jnp.arange(length, dtype=jnp.int32)
    causal = (places[:, None] >= places[None, :])[:, :, None]
    spread = jnp.where(causal, log_decay[:, None, :] - log_decay[None, :, :], 0.0)
    decays = jnp.where(causal, jnp.exp(spread), 0.0)
    coupling = jnp.einsum('tgn,sgn->gts', c_state, b_state, precision=HIGHEST)
    coupling = jnp.repeat(coupling, group_heads, axis=0)
    mixing = jnp.transpose(decays, (2, 0, 1)) * coupling
    scaled = signal * step_size[:, :, None]
    output = jnp.einsum('hts,shp->thp', mixing, scaled, precision=HIGHEST)
    b_heads = jnp.repeat(b_state, group_heads, axis=1)
    c_heads = jnp.repeat(c_state, group_heads, axis=1)
    output = output + jnp.exp(log_decay)[:, :, None] * jnp.einsum('thn,hpn->thp', c_heads, carried, precision=HIGHEST)
    closing = jnp.exp(log_decay[-1][None, :] - log_decay)
    weighted = scaled * closing[:, :, None]
    updated = jnp.exp(log_decay[-1])[:, None, None] * carried + jnp.einsum('shp,shn->hpn', weighted, b_heads, precision=HIGHEST)
    return (output, updated, log_decay, c_heads)

def attend_update(carry, query_block, query_start, key_block, value_block, key_start, widen):
    maxima, totals, accum = carry
    kv_heads = key_block.shape[1] // HD
    grouped = query_block.shape[1] // HD // kv_heads
    query_rows = query_block.shape[0]
    key_rows = key_block.shape[0]
    query_four = query_block.reshape(query_rows, kv_heads, grouped, HD)
    key_three = key_block.reshape(key_rows, kv_heads, HD)
    value_three = value_block.reshape(key_rows, kv_heads, HD)
    if widen:
        scores = jnp.einsum('qhgd,khd->hgqk', query_four.astype(jnp.float32), key_three.astype(jnp.float32))
    else:
        scores = jnp.einsum('qhgd,khd->hgqk', query_four, key_three, preferred_element_type=jnp.float32)
    scores = scores * (1.0 / math.sqrt(HD))
    query_places = query_start + jnp.arange(query_rows, dtype=jnp.int32)
    key_places = key_start + jnp.arange(key_rows, dtype=jnp.int32)
    allowed = key_places[None, :] <= query_places[:, None]
    masked = jnp.where(allowed, scores, lowest_score)
    newmax = jnp.maximum(maxima, lax.optimization_barrier(jnp.max(masked, axis=-1)))
    probs = jnp.where(allowed, jnp.exp(masked - newmax[..., None]), 0.0)
    factor = jnp.exp(maxima - newmax)
    totals = totals * factor + lax.optimization_barrier(jnp.sum(probs, axis=-1))
    rounded = probs.astype(jnp.bfloat16)
    if widen:
        product = jnp.einsum('hgqk,khd->hgqd', rounded.astype(jnp.float32), value_three.astype(jnp.float32))
    else:
        product = jnp.einsum('hgqk,khd->hgqd', rounded, value_three, preferred_element_type=jnp.float32)
    accum = accum * factor[..., None] + product
    return (newmax, totals, accum)

def finish(carry):
    maxima, totals, accum = carry
    result = accum / totals[..., None]
    result = jnp.transpose(result, (2, 0, 1, 3))
    return result.reshape(result.shape[0], -1).astype(jnp.bfloat16)

def attention(queries, keys, values):
    span = math.gcd(TOKENS, 512)
    count = TOKENS // span
    grouped = QH // KVH

    def one_block(index):
        start = index * span
        query_block = lax.dynamic_slice_in_dim(queries, start, span, 0)
        initial = (jnp.full((KVH, grouped, span), lowest_score, jnp.float32), jnp.zeros((KVH, grouped, span), jnp.float32), jnp.zeros((KVH, grouped, span, HD), jnp.float32))

        def visit(position, carry):
            key_start = position * span
            key_block = lax.dynamic_slice_in_dim(keys, key_start, span, 0)
            value_block = lax.dynamic_slice_in_dim(values, key_start, span, 0)
            return attend_update(carry, query_block, start, key_block, value_block, key_start, True)
        return finish(lax.fori_loop(0, index + 1, visit, initial))
    blocks = lax.map(one_block, jnp.arange(count, dtype=jnp.int32))
    return blocks.reshape(TOKENS, QH * HD)

def reference(mixer_input, gate_input, input_matrix, output_matrix, step_raw, step_bias, decay_rate, skip_weight, conv_mixer, conv_input, conv_output, norm_gain, queries, keys, values):
    reach = CONV - 1
    signal = conv_silu(mixer_input, conv_mixer, jnp.zeros((reach, mixer_input.shape[1]), jnp.bfloat16))
    b_state = conv_silu(input_matrix, conv_input, jnp.zeros((reach, input_matrix.shape[1]), jnp.bfloat16))
    c_state = conv_silu(output_matrix, conv_output, jnp.zeros((reach, output_matrix.shape[1]), jnp.bfloat16))
    signal = signal.reshape(TOKENS, MH, P_SIZE)
    b_state = b_state.reshape(TOKENS, GROUPS, STATE)
    c_state = c_state.reshape(TOKENS, GROUPS, STATE)
    step_size = jax.nn.softplus(step_raw + step_bias[None, :])
    blocks = TOKENS // SCAN_BLOCK

    def advance(carried, pieces):
        signal_part, b_part, c_part, step_part = pieces
        output, updated, log_decay, c_heads = ssd_block(signal_part, b_part, c_part, step_part, decay_rate, carried)
        return (updated, output)
    _, outputs = lax.scan(advance, jnp.zeros((MH, P_SIZE, STATE), jnp.float32), (signal.reshape(blocks, SCAN_BLOCK, MH, P_SIZE), b_state.reshape(blocks, SCAN_BLOCK, GROUPS, STATE), c_state.reshape(blocks, SCAN_BLOCK, GROUPS, STATE), step_size.reshape(blocks, SCAN_BLOCK, MH)))
    mixed = outputs.reshape(TOKENS, MH, P_SIZE) + skip_weight[None, :, None] * signal
    gated = mixed.reshape(TOKENS, MH * P_SIZE) * jax.nn.silu(gate_input.astype(jnp.float32))
    squares = lax.optimization_barrier(jnp.mean(gated * gated, axis=1, keepdims=True))
    mixer_out = (gated * lax.rsqrt(squares + norm_epsilon) * norm_gain[None, :]).astype(jnp.bfloat16)
    attention_out = attention(queries, keys, values)
    return (mixer_out, attention_out)
```

```python
import functools
import math

import jax
import jax.numpy as jnp
from jax import lax
from jax.experimental import pallas as pl
from jax.experimental.pallas import tpu as pltpu
from jax.sharding import Mesh
from jax.sharding import PartitionSpec as P

P_SIZE = 64
STATE = 128
HD = 128
CONV = 4
SEQ = ("seq_0", "seq_1", "seq_2")
MESH = pl.DeviceIdType.MESH
F32 = jnp.float32
BF16 = jnp.bfloat16
HIGHEST = lax.Precision.HIGHEST
EPSILON = 1e-05
LOWEST = -1e30
KEY_TILE = 512
ROWS = 256
TAIL = 16


def nt(a, b, precision=None):
    return lax.dot_general(
        a, b, (((1,), (1,)), ((), ())), preferred_element_type=F32, precision=precision
    )


def nn(a, b, precision=None):
    return lax.dot_general(
        a, b, (((1,), (0,)), ((), ())), preferred_element_type=F32, precision=precision
    )


def silu(a):
    return a / (1.0 + jnp.exp(-a))


def two_parts(value):
    high = value.astype(BF16)
    low = (value - high.astype(F32)).astype(BF16)
    return high, low


def kernel(
    dims,
    x_ref,
    gate_ref,
    b_ref,
    c_ref,
    step_ref,
    bias_ref,
    rate_ref,
    skip_ref,
    wx_ref,
    wb_ref,
    wc_ref,
    gain_ref,
    q_ref,
    k_ref,
    v_ref,
    mixer_ref,
    attn_ref,
    tail_x,
    tail_b,
    tail_c,
    pad_x,
    pad_s,
    signal,
    scaled,
    entry_decay,
    skip_rows,
    b_turned,
    b_held,
    c_held,
    log_held,
    logt_held,
    state_out,
    decay_out,
    state_in,
    decay_in,
    prefix,
    total_out,
    total_decay_out,
    total_in,
    total_decay_in,
    enter_out,
    enter_in,
    diagonal,
    gated,
    squares,
    kv,
    q_far,
    q_rows,
    o_far,
    o_in,
    m_held,
    acc_held,
    tail_send,
    tail_recv,
    pair_send,
    pair_recv,
    ring_send,
    ring_recv,
    row_send,
    row_recv,
    a2a_send,
    a2a_recv,
    tot_send,
    tot_recv,
    back_send,
    back_recv,
    sq_send,
    sq_recv,
):
    Y, Z, TP = dims
    T = x_ref.shape[0]
    HW = x_ref.shape[1]
    heads = HW // P_SIZE
    W = HW // Z
    G = b_ref.shape[1] // STATE
    GW = HW // G
    YZ = Y * Z
    QW = q_ref.shape[1] // 2
    grouped = QW // HD

    x = lax.axis_index("seq_0")
    y = lax.axis_index("seq_1")
    z = lax.axis_index("seq_2")
    t = lax.axis_index("tp")
    seq = x * YZ + y * Z + z
    count = 2 * YZ

    def place(index):
        return (index // YZ, (index // Z) % Y, index % Z, t)

    after = place((seq + 1) % count)
    before = place((seq + count - 1) % count)
    partner = (1 - x, Y - 1 - y, z, t)

    def z_peer(d):
        return (x, y, (z + d) % Z, t)

    def y_peer(d):
        return (x, (y + d) % Y, z, t)

    group = x * Y + y

    def group_peer(d):
        other = (group + d) % (2 * Y)
        return (other // Y, other % Y, z, t)

    def tp_peer(d):
        return (x, y, z, (t + d) % TP)

    barrier = pltpu.get_barrier_semaphore()
    greeted = [after, before]
    greeted += [z_peer(d) for d in range(1, Z)]
    greeted += [group_peer(d) for d in range(1, 2 * Y)]
    greeted += [tp_peer(d) for d in range(1, TP)]
    for peer in greeted:
        pl.semaphore_signal(barrier, inc=1, device_id=peer, device_id_type=MESH)

    def remote(src, dst, send, recv, peer):
        return pltpu.make_async_remote_copy(
            src_ref=src,
            dst_ref=dst,
            send_sem=send,
            recv_sem=recv,
            device_id=peer,
            device_id_type=MESH,
        )

    sent = []

    def start(src, dst, send, recv, peer):
        copy = remote(src, dst, send, recv, peer)
        copy.start()
        sent.append(copy)

    def arrived(dst, send, recv, peer):
        remote(dst, dst, send, recv, peer).wait_recv()

    def block_of(half, yy, zz):
        if half == 0:
            return x * YZ + yy * Z + zz
        return (1 - x) * YZ + (Y - 1 - yy) * Z + zz

    def kv_at(half, yy, zz):
        return kv.at[:, pl.ds(pl.multiple_of(block_of(half, yy, zz) * T, T), T), :]

    own_rows = pl.ds(pl.multiple_of(block_of(0, y, z) * T, T), T)
    kv[0, own_rows, :] = k_ref[:, pl.ds(pl.multiple_of(x * HD, HD), HD)]
    kv[1, own_rows, :] = v_ref[:, pl.ds(pl.multiple_of(x * HD, HD), HD)]
    for h in range(grouped):
        q_rows[0, h * T : (h + 1) * T, :] = q_ref[
            :, pl.ds(pl.multiple_of(x * QW + h * HD, HD), HD)
        ]

    step_in = step_ref[...] + bias_ref[...]
    step = jnp.maximum(step_in, 0.0) + jnp.log(1.0 + jnp.exp(-jnp.abs(step_in)))
    rows_at = lax.broadcasted_iota(jnp.int32, (T, T), 0)
    cols_at = lax.broadcasted_iota(jnp.int32, (T, T), 1)
    lower = jnp.where(rows_at >= cols_at, 1.0, 0.0).astype(F32)
    wide = jnp.concatenate(
        [-step * rate_ref[...], jnp.zeros((T, STATE - heads), F32)], axis=1
    )
    log_decay = nn(lower, wide, HIGHEST)
    log_held[...] = log_decay
    logt_held[...] = log_decay.T
    log_decay = log_decay[:, :heads]
    last = log_decay[T - 1 : T, :]
    closing = jnp.exp(last - log_decay)
    columns = jnp.concatenate([step, step * closing, jnp.exp(log_decay)], axis=0)
    columns_high, columns_low = two_parts(columns)
    whole = jnp.concatenate(
        [
            jnp.broadcast_to(jnp.exp(last), (8, heads)),
            jnp.broadcast_to(skip_ref[...], (8, heads)),
        ],
        axis=0,
    )
    whole_high, whole_low = two_parts(whole)

    pl.semaphore_wait(barrier, len(greeted))

    start(x_ref.at[T - TAIL :, :], tail_x, tail_send.at[0], tail_recv.at[0], after)
    start(b_ref.at[T - TAIL :, :], tail_b, tail_send.at[1], tail_recv.at[1], after)
    start(c_ref.at[T - TAIL :, :], tail_c, tail_send.at[2], tail_recv.at[2], after)
    far_cols = pl.ds(pl.multiple_of((1 - x) * HD, HD), HD)
    for i, ref in enumerate((k_ref, v_ref)):
        start(
            ref.at[:, far_cols],
            kv.at[i, own_rows, :],
            pair_send.at[i],
            pair_recv.at[i],
            partner,
        )

    right_steps = Z // 2
    left_steps = (Z - 1) // 2

    def ring_start(half, s):
        if s < right_steps:
            piece = kv_at(half, y, (z + Z - s) % Z)
            start(piece, piece, ring_send.at[half, 0, s], ring_recv.at[half, 0, s], z_peer(1))
        if s < left_steps:
            piece = kv_at(half, y, (z + s) % Z)
            start(piece, piece, ring_send.at[half, 1, s], ring_recv.at[half, 1, s], z_peer(Z - 1))

    def ring_wait(half, s):
        if s < right_steps:
            piece = kv_at(half, y, (z + Z - 1 - s) % Z)
            arrived(piece, ring_send.at[half, 0, s], ring_recv.at[half, 0, s], z_peer(Z - 1))
        if s < left_steps:
            piece = kv_at(half, y, (z + 1 + s) % Z)
            arrived(piece, ring_send.at[half, 1, s], ring_recv.at[half, 1, s], z_peer(1))

    def row_start(half, d):
        piece = kv_at(half, y, (z + d) % Z)
        if Y > 1:
            start(piece, piece, row_send.at[half, 0, d], row_recv.at[half, 0, d], y_peer(1))
        if Y > 2:
            start(piece, piece, row_send.at[half, 1, d], row_recv.at[half, 1, d], y_peer(Y - 1))

    def row_forward(half, d):
        if Y > 1:
            piece = kv_at(half, (y + Y - 1) % Y, (z + d) % Z)
            arrived(piece, row_send.at[half, 0, d], row_recv.at[half, 0, d], y_peer(Y - 1))
            if Y > 3 and 2 * d < Z:
                start(piece, piece, row_send.at[half, 2, d], row_recv.at[half, 2, d], y_peer(1))
        if Y > 2:
            piece = kv_at(half, (y + 1) % Y, (z + d) % Z)
            arrived(piece, row_send.at[half, 1, d], row_recv.at[half, 1, d], y_peer(1))
            if Y > 3 and 2 * d >= Z:
                start(
                    piece, piece, row_send.at[half, 2, d], row_recv.at[half, 2, d], y_peer(Y - 1)
                )

    def row_last(half, d):
        if Y > 3:
            piece = kv_at(half, (y + 2) % Y, (z + d) % Z)
            arrived(
                piece,
                row_send.at[half, 2, d],
                row_recv.at[half, 2, d],
                y_peer(Y - 1 if 2 * d < Z else 1),
            )

    def offsets(s):
        found = []
        if s < right_steps:
            found.append(Z - 1 - s)
        if s < left_steps:
            found.append(1 + s)
        return found

    ring_start(0, 0)
    row_start(0, 0)
    start(
        q_ref.at[:, pl.ds(pl.multiple_of((1 - x) * QW, QW), QW)],
        q_far,
        pair_send.at[2],
        pair_recv.at[2],
        partner,
    )

    arrived(tail_x, tail_send.at[0], tail_recv.at[0], before)
    arrived(tail_b, tail_send.at[1], tail_recv.at[1], before)
    arrived(tail_c, tail_send.at[2], tail_recv.at[2], before)
    inside = jnp.where(seq > 0, 1.0, 0.0).astype(F32)

    def conv_silu(pad, tail, rows, weights):
        pad[0:8, :] = tail[8:16, :].astype(F32) * inside
        pad[8 : T + 8, :] = rows.astype(F32)
        total = weights[0:1, :] * pad[5 : T + 5, :]
        for k in range(1, CONV):
            total = total + weights[k : k + 1, :] * pad[5 + k : T + 5 + k, :]
        return silu(total)

    for g in range(G):
        cols = slice(g * STATE, (g + 1) * STATE)
        b_now = conv_silu(pad_s, tail_b[:, cols], b_ref[:, cols], wb_ref[:, cols])
        b_held[g] = b_now.astype(BF16)
        b_turned[g] = b_now.T.astype(BF16)
        c_now = conv_silu(pad_s, tail_c[:, cols], c_ref[:, cols], wc_ref[:, cols])
        c_held[g] = c_now.astype(BF16)

    for d in [*range(1, Z), 0]:
        k = (z + d) % Z
        at = pl.ds(pl.multiple_of(k * W, W), W)
        spread = jnp.where(
            lax.broadcasted_iota(jnp.int32, (heads, W), 0)
            == k * (W // P_SIZE) + lax.broadcasted_iota(jnp.int32, (heads, W), 1) // P_SIZE,
            1.0,
            0.0,
        ).astype(BF16)
        per_lane = nn(columns_high, spread) + nn(columns_low, spread)
        per_whole = nn(whole_high, spread) + nn(whole_low, spread)
        now = conv_silu(pad_x, tail_x[:, at], x_ref[:, at], wx_ref[:, at])
        signal[:, at] = now
        scaled[:, at] = (now * per_lane[:T]).astype(BF16)
        entry_decay[:, at] = per_lane[2 * T :]
        skip_rows[:, at] = per_whole[8:]
        weighted = (now * per_lane[T : 2 * T]).astype(BF16)
        state = nn(b_turned[k * W // GW], weighted)
        if d:
            state_out[d] = state.astype(BF16)
            decay_out[d] = per_whole[:8]
            start(state_out.at[d], state_in.at[z], a2a_send.at[0, d], a2a_recv.at[0, d], z_peer(d))
            start(decay_out.at[d], decay_in.at[z], a2a_send.at[1, d], a2a_recv.at[1, d], z_peer(d))
        else:
            state_in[z] = state.astype(BF16)
            decay_in[z] = per_whole[:8]

    for i in range(2):
        arrived(
            kv.at[i, pl.ds(pl.multiple_of(block_of(1, y, z) * T, T), T), :],
            pair_send.at[i],
            pair_recv.at[i],
            partner,
        )
    ring_start(1, 0)
    row_start(1, 0)

    causal = rows_at >= cols_at
    couplings = [nt(c_held[g], b_held[g]) for g in range(G)]
    lane_at = lax.broadcasted_iota(jnp.int32, (T, 2 * P_SIZE), 1)

    def pair_of_heads(p):
        mixes = []
        for h in (2 * p, 2 * p + 1):
            spread = log_held[:, h : h + 1] - logt_held[h : h + 1, :]
            decays = jnp.exp(jnp.where(causal, spread, LOWEST))
            mixes.append((decays * couplings[h * P_SIZE // GW]).astype(BF16))
        two = scaled[:, p * 128 : (p + 1) * 128]
        zero = jnp.zeros_like(two)
        stacked = jnp.concatenate(
            [jnp.where(lane_at < P_SIZE, two, zero), jnp.where(lane_at < P_SIZE, zero, two)],
            axis=0,
        )
        diagonal[:, p * 128 : (p + 1) * 128] = nn(jnp.concatenate(mixes, axis=1), stacked)

    pairs = heads // 2
    steps = max(right_steps, 1)
    for s in range(steps):
        for p in range(s * pairs // steps, (s + 1) * pairs // steps):
            pair_of_heads(p)
        for half in range(2):
            if s < right_steps:
                ring_wait(half, s)
                if s + 1 < right_steps:
                    ring_start(half, s + 1)
                for d in offsets(s):
                    row_start(half, d)

    for d in range(1, Z):
        source = (z + Z - d) % Z
        arrived(state_in.at[source], a2a_send.at[0, d], a2a_recv.at[0, d], z_peer(Z - d))
        arrived(decay_in.at[source], a2a_send.at[1, d], a2a_recv.at[1, d], z_peer(Z - d))
    running = jnp.zeros((STATE, W), F32)
    running_decay = jnp.ones((8, W), F32)
    for i in range(Z):
        prefix[i] = running
        keep = decay_in[i]
        running = running * keep[0:1] + state_in[i].astype(F32)
        running_decay = running_decay * keep
    total_out[...] = running.astype(BF16)
    total_decay_out[...] = running_decay
    total_in[group] = running.astype(BF16)
    total_decay_in[group] = running_decay
    for d in range(1, 2 * Y):
        start(total_out, total_in.at[group], tot_send.at[0, d], tot_recv.at[0, d], group_peer(d))
        start(
            total_decay_out,
            total_decay_in.at[group],
            tot_send.at[1, d],
            tot_recv.at[1, d],
            group_peer(d),
        )

    for d in range(Z):
        for half in range(2):
            row_forward(half, d)

    for d in range(1, 2 * Y):
        source = (group + 2 * Y - d) % (2 * Y)
        arrived(total_in.at[source], tot_send.at[0, d], tot_recv.at[0, d], group_peer(2 * Y - d))
        arrived(
            total_decay_in.at[source], tot_send.at[1, d], tot_recv.at[1, d], group_peer(2 * Y - d)
        )
    entering = jnp.zeros((STATE, W), F32)
    for i in range(2 * Y):
        further = entering * total_decay_in[i][0:1] + total_in[i].astype(F32)
        entering = jnp.where(i < group, further, entering)
    so_far = jnp.ones((8, W), F32)
    for i in range(Z):
        enter_out[i] = (prefix[i] + entering * so_far[0:1]).astype(BF16)
        so_far = so_far * decay_in[i]
    for d in range(1, Z):
        k = (z + d) % Z
        start(enter_out.at[k], enter_in.at[z], back_send.at[d], back_recv.at[d], z_peer(d))
    enter_in[z] = enter_out[z]

    for d in range(Z):
        for half in range(2):
            row_last(half, d)
    arrived(q_far, pair_send.at[2], pair_recv.at[2], partner)
    for h in range(grouped):
        q_rows[1, h * T : (h + 1) * T, :] = q_far[:, h * HD : (h + 1) * HD]

    scale = math.log2(math.e) / math.sqrt(HD)
    all_rows = grouped * T
    chunk = min(ROWS, all_rows)

    def attend(which, position):
        m_held[...] = jnp.full(m_held.shape, LOWEST, F32)
        acc_held[...] = jnp.zeros(acc_held.shape, F32)

        def tile(index, masked):
            keys_at = pl.ds(pl.multiple_of(index * KEY_TILE, KEY_TILE), KEY_TILE)
            keys = kv[0, keys_at, :]
            values = jnp.concatenate([kv[1, keys_at, :], jnp.ones((KEY_TILE, HD), BF16)], axis=1)
            for r in range(0, all_rows, chunk):
                scores = nt(q_rows[which, r : r + chunk, :], keys)
                if masked:
                    row = lax.broadcasted_iota(jnp.int32, (chunk, KEY_TILE), 0) % T
                    col = lax.broadcasted_iota(jnp.int32, (chunk, KEY_TILE), 1)
                    scores = jnp.where(
                        col + index * KEY_TILE <= row + position * T, scores, LOWEST
                    )
                old = m_held[r : r + chunk, :]
                new = jnp.maximum(old, jnp.max(scores, axis=1, keepdims=True))
                m_held[r : r + chunk, :] = new
                factor = jnp.exp2((old - new) * scale)
                weights = jnp.concatenate(
                    [
                        jnp.exp2((scores[:, j : j + HD] - new) * scale).astype(BF16)
                        for j in range(0, KEY_TILE, HD)
                    ],
                    axis=1,
                )
                product = nn(weights, values)
                acc_held[r : r + chunk, :] = (
                    acc_held[r : r + chunk, :] * jnp.concatenate([factor, factor], axis=1)
                    + product
                )

        full = position * T // KEY_TILE
        lax.fori_loop(0, full, lambda i, n: (tile(i, False), n)[1], 0)
        tile(full, True)

    def result(h):
        both = acc_held[h * T : (h + 1) * T, :]
        return (both[:, :HD] / both[:, HD:]).astype(BF16)

    attend(1, block_of(1, y, z))
    for h in range(grouped):
        o_far[:, h * HD : (h + 1) * HD] = result(h)
    start(o_far, o_in, pair_send.at[3], pair_recv.at[3], partner)
    attend(0, seq)
    for h in range(grouped):
        attn_ref[:, pl.ds(pl.multiple_of(x * QW + h * HD, HD), HD)] = result(h)

    for d in range(1, Z):
        source = (z + Z - d) % Z
        arrived(enter_in.at[source], back_send.at[d], back_recv.at[d], z_peer(Z - d))
    summed = jnp.zeros((T, 128), F32)
    for k in range(Z):
        cols = slice(k * W, (k + 1) * W)
        off = nn(c_held[k * W // GW], enter_in[k])
        mixed = diagonal[:, cols] + entry_decay[:, cols] * off
        mixed = mixed + skip_rows[0:1, cols] * signal[:, cols]
        now = mixed * silu(gate_ref[:, cols].astype(F32))
        gated[:, cols] = now
        now = now * now
        for j in range(0, W, 128):
            summed = summed + now[:, j : j + 128]
    squares[t] = nt(jnp.ones((8, 128), F32), summed, HIGHEST)
    for d in range(1, TP):
        start(squares.at[t], squares.at[t], sq_send.at[d], sq_recv.at[d], tp_peer(d))
    for d in range(1, TP):
        source = (t + TP - d) % TP
        arrived(squares.at[source], sq_send.at[d], sq_recv.at[d], tp_peer(TP - d))
    everything = squares[0]
    for i in range(1, TP):
        everything = everything + squares[i]
    everything = jnp.broadcast_to(everything[0:1, :], (T, T)).T
    factor = lax.rsqrt(everything / (HW * TP) + EPSILON)
    for j in range(0, HW, 128):
        mixer_ref[:, j : j + 128] = (
            gated[:, j : j + 128] * factor * gain_ref[:, j : j + 128]
        ).astype(BF16)

    arrived(o_in, pair_send.at[3], pair_recv.at[3], partner)
    attn_ref[:, pl.ds(pl.multiple_of((1 - x) * QW, QW), QW)] = o_in[...]
    for copy in sent:
        copy.wait_send()


def shards(dims, *args):
    (x, gate, b, c, step, bias, rate, skip, wx, wb, wc, gain, q, k, v) = args
    bias, rate, skip, gain = (a.reshape(1, -1) for a in (bias, rate, skip, gain))
    Y, Z, TP = dims
    T, HW = x.shape
    W = HW // Z
    G = b.shape[1] // STATE
    count = 2 * Y * Z
    QW = q.shape[1] // 2
    rows = QW // HD * T
    vmem, dma = pltpu.VMEM, pltpu.SemaphoreType.DMA
    scratch = [
        vmem((TAIL, HW), BF16),
        vmem((TAIL, G * STATE), BF16),
        vmem((TAIL, G * STATE), BF16),
        vmem((T + 8, W), F32),
        vmem((T + 8, STATE), F32),
        vmem((T, HW), F32),
        vmem((T, HW), BF16),
        vmem((T, HW), F32),
        vmem((8, HW), F32),
        vmem((G, STATE, T), BF16),
        vmem((G, T, STATE), BF16),
        vmem((G, T, STATE), BF16),
        vmem((T, STATE), F32),
        vmem((STATE, T), F32),
        vmem((Z, STATE, W), BF16),
        vmem((Z, 8, W), F32),
        vmem((Z, STATE, W), BF16),
        vmem((Z, 8, W), F32),
        vmem((Z, STATE, W), F32),
        vmem((STATE, W), BF16),
        vmem((8, W), F32),
        vmem((2 * Y, STATE, W), BF16),
        vmem((2 * Y, 8, W), F32),
        vmem((Z, STATE, W), BF16),
        vmem((Z, STATE, W), BF16),
        vmem((T, HW), F32),
        vmem((T, HW), F32),
        vmem((TP, 8, 128), F32),
        vmem((2, count * T, HD), BF16),
        vmem((T, QW), BF16),
        vmem((2, rows, HD), BF16),
        vmem((T, QW), BF16),
        vmem((T, QW), BF16),
        vmem((rows, HD), F32),
        vmem((rows, 2 * HD), F32),
        dma((3,)),
        dma((3,)),
        dma((4,)),
        dma((4,)),
        dma((2, 2, max(Z // 2, 1))),
        dma((2, 2, max(Z // 2, 1))),
        dma((2, 3, Z)),
        dma((2, 3, Z)),
        dma((2, Z)),
        dma((2, Z)),
        dma((2, 2 * Y)),
        dma((2, 2 * Y)),
        dma((Z,)),
        dma((Z,)),
        dma((TP,)),
        dma((TP,)),
    ]
    whole = pl.BlockSpec(memory_space=pltpu.VMEM)
    return pl.pallas_call(
        functools.partial(kernel, dims),
        out_shape=(
            jax.ShapeDtypeStruct((T, HW), BF16),
            jax.ShapeDtypeStruct((T, 2 * QW), BF16),
        ),
        in_specs=[whole] * 15,
        out_specs=(whole, whole),
        scratch_shapes=scratch,
        compiler_params=pltpu.CompilerParams(
            collective_id=0, has_side_effects=True, vmem_limit_bytes=60 * 1024 * 1024
        ),
        name="hybrid",
    )(x, gate, b, c, step, bias, rate, skip, wx, wb, wc, gain, q, k, v)


def build(mesh, Y, Z):
    TP = mesh.shape["tp"]
    torus = Mesh(mesh.devices.reshape(2, Y, Z, TP), (*SEQ, "tp"))
    cut, by_tp = P(SEQ, "tp"), P("tp")
    taps = P(None, "tp")
    placed = (cut,) * 5 + (by_tp,) * 3 + (taps,) * 3 + (by_tp,) + (cut,) * 3
    return jax.shard_map(
        functools.partial(shards, (Y, Z, TP)),
        mesh=torus,
        in_specs=placed,
        out_specs=(cut, cut),
        check_vma=False,
    )


def solution(mesh):
    return build(mesh, 4, 8)
```

```python
import functools
import math

import jax
import jax.numpy as jnp
from jax import lax
from jax.experimental import pallas as pl
from jax.experimental.pallas import tpu as pltpu
from jax.sharding import Mesh
from jax.sharding import PartitionSpec as P

P_SIZE = 64
STATE = 128
HD = 128
CONV = 4
SEQ = ("seq_0", "seq_1", "seq_2")
MESH = pl.DeviceIdType.MESH
F32 = jnp.float32
BF16 = jnp.bfloat16
HIGHEST = lax.Precision.HIGHEST
EPSILON = 1e-05
LOWEST = -1e30
KEY_TILE = 512
ROWS = 256
TAIL = 16


def nt(a, b, precision=None):
    return lax.dot_general(
        a, b, (((1,), (1,)), ((), ())), preferred_element_type=F32, precision=precision
    )


def nn(a, b, precision=None):
    return lax.dot_general(
        a, b, (((1,), (0,)), ((), ())), preferred_element_type=F32, precision=precision
    )


def silu(a):
    return a / (1.0 + jnp.exp(-a))


def two_parts(value):
    high = value.astype(BF16)
    low = (value - high.astype(F32)).astype(BF16)
    return high, low


def kernel(
    dims,
    x_ref,
    gate_ref,
    b_ref,
    c_ref,
    step_ref,
    bias_ref,
    rate_ref,
    skip_ref,
    wx_ref,
    wb_ref,
    wc_ref,
    gain_ref,
    q_ref,
    k_ref,
    v_ref,
    mixer_ref,
    attn_ref,
    tail_x,
    tail_b,
    tail_c,
    pad_x,
    pad_s,
    signal,
    scaled,
    entry_decay,
    skip_rows,
    b_turned,
    b_held,
    c_held,
    log_held,
    logt_held,
    state_out,
    decay_out,
    state_in,
    decay_in,
    prefix,
    total_out,
    total_decay_out,
    total_in,
    total_decay_in,
    enter_out,
    enter_in,
    diagonal,
    gated,
    squares,
    kv,
    q_far,
    q_rows,
    o_far,
    o_in,
    m_held,
    acc_held,
    tail_send,
    tail_recv,
    pair_send,
    pair_recv,
    ring_send,
    ring_recv,
    row_send,
    row_recv,
    a2a_send,
    a2a_recv,
    tot_send,
    tot_recv,
    back_send,
    back_recv,
    sq_send,
    sq_recv,
):
    Y, Z, TP = dims
    T = x_ref.shape[0]
    HW = x_ref.shape[1]
    heads = HW // P_SIZE
    W = HW // Z
    G = b_ref.shape[1] // STATE
    GW = HW // G
    YZ = Y * Z
    QW = q_ref.shape[1] // 2
    grouped = QW // HD

    x = lax.axis_index("seq_0")
    y = lax.axis_index("seq_1")
    z = lax.axis_index("seq_2")
    t = lax.axis_index("tp")
    seq = x * YZ + y * Z + z
    count = 2 * YZ

    def place(index):
        return (index // YZ, (index // Z) % Y, index % Z, t)

    after = place((seq + 1) % count)
    before = place((seq + count - 1) % count)
    partner = (1 - x, Y - 1 - y, z, t)

    def z_peer(d):
        return (x, y, (z + d) % Z, t)

    def y_peer(d):
        return (x, (y + d) % Y, z, t)

    group = x * Y + y

    def group_peer(d):
        other = (group + d) % (2 * Y)
        return (other // Y, other % Y, z, t)

    def tp_peer(d):
        return (x, y, z, (t + d) % TP)

    barrier = pltpu.get_barrier_semaphore()
    greeted = [after, before]
    greeted += [z_peer(d) for d in range(1, Z)]
    greeted += [group_peer(d) for d in range(1, 2 * Y)]
    greeted += [tp_peer(d) for d in range(1, TP)]
    for peer in greeted:
        pl.semaphore_signal(barrier, inc=1, device_id=peer, device_id_type=MESH)

    def remote(src, dst, send, recv, peer):
        return pltpu.make_async_remote_copy(
            src_ref=src,
            dst_ref=dst,
            send_sem=send,
            recv_sem=recv,
            device_id=peer,
            device_id_type=MESH,
        )

    sent = []

    def start(src, dst, send, recv, peer):
        copy = remote(src, dst, send, recv, peer)
        copy.start()
        sent.append(copy)

    def arrived(dst, send, recv, peer):
        remote(dst, dst, send, recv, peer).wait_recv()

    def block_of(half, yy, zz):
        if half == 0:
            return x * YZ + yy * Z + zz
        return (1 - x) * YZ + (Y - 1 - yy) * Z + zz

    def kv_at(half, yy, zz):
        return kv.at[:, pl.ds(pl.multiple_of(block_of(half, yy, zz) * T, T), T), :]

    own_rows = pl.ds(pl.multiple_of(block_of(0, y, z) * T, T), T)
    kv[0, own_rows, :] = k_ref[:, pl.ds(pl.multiple_of(x * HD, HD), HD)]
    kv[1, own_rows, :] = v_ref[:, pl.ds(pl.multiple_of(x * HD, HD), HD)]
    for h in range(grouped):
        q_rows[0, h * T : (h + 1) * T, :] = q_ref[
            :, pl.ds(pl.multiple_of(x * QW + h * HD, HD), HD)
        ]

    turned = jnp.concatenate(
        [step_ref[...], jnp.zeros((STATE - heads, T), F32)], axis=0
    ).T
    step_in = turned[:, :heads] + bias_ref[...]
    step = jnp.maximum(step_in, 0.0) + jnp.log(1.0 + jnp.exp(-jnp.abs(step_in)))
    rows_at = lax.broadcasted_iota(jnp.int32, (T, T), 0)
    cols_at = lax.broadcasted_iota(jnp.int32, (T, T), 1)
    lower = jnp.where(rows_at >= cols_at, 1.0, 0.0).astype(F32)
    wide = jnp.concatenate(
        [-step * rate_ref[...], jnp.zeros((T, STATE - heads), F32)], axis=1
    )
    log_decay = nn(lower, wide, HIGHEST)
    log_held[...] = log_decay
    logt_held[...] = log_decay.T
    log_decay = log_decay[:, :heads]
    last = log_decay[T - 1 : T, :]
    closing = jnp.exp(last - log_decay)
    columns = jnp.concatenate([step, step * closing, jnp.exp(log_decay)], axis=0)
    columns_high, columns_low = two_parts(columns)
    whole = jnp.concatenate(
        [
            jnp.broadcast_to(jnp.exp(last), (8, heads)),
            jnp.broadcast_to(skip_ref[...], (8, heads)),
        ],
        axis=0,
    )
    whole_high, whole_low = two_parts(whole)

    pl.semaphore_wait(barrier, len(greeted))

    start(x_ref.at[T - TAIL :, :], tail_x, tail_send.at[0], tail_recv.at[0], after)
    start(b_ref.at[T - TAIL :, :], tail_b, tail_send.at[1], tail_recv.at[1], after)
    start(c_ref.at[T - TAIL :, :], tail_c, tail_send.at[2], tail_recv.at[2], after)
    far_cols = pl.ds(pl.multiple_of((1 - x) * HD, HD), HD)
    for i, ref in enumerate((k_ref, v_ref)):
        start(
            ref.at[:, far_cols],
            kv.at[i, own_rows, :],
            pair_send.at[i],
            pair_recv.at[i],
            partner,
        )

    right_steps = Z // 2
    left_steps = (Z - 1) // 2

    def ring_start(half, s):
        if s < right_steps:
            piece = kv_at(half, y, (z + Z - s) % Z)
            start(piece, piece, ring_send.at[half, 0, s], ring_recv.at[half, 0, s], z_peer(1))
        if s < left_steps:
            piece = kv_at(half, y, (z + s) % Z)
            start(piece, piece, ring_send.at[half, 1, s], ring_recv.at[half, 1, s], z_peer(Z - 1))

    def ring_wait(half, s):
        if s < right_steps:
            piece = kv_at(half, y, (z + Z - 1 - s) % Z)
            arrived(piece, ring_send.at[half, 0, s], ring_recv.at[half, 0, s], z_peer(Z - 1))
        if s < left_steps:
            piece = kv_at(half, y, (z + 1 + s) % Z)
            arrived(piece, ring_send.at[half, 1, s], ring_recv.at[half, 1, s], z_peer(1))

    def row_start(half, d):
        piece = kv_at(half, y, (z + d) % Z)
        if Y > 1:
            start(piece, piece, row_send.at[half, 0, d], row_recv.at[half, 0, d], y_peer(1))
        if Y > 2:
            start(piece, piece, row_send.at[half, 1, d], row_recv.at[half, 1, d], y_peer(Y - 1))

    def row_forward(half, d):
        if Y > 1:
            piece = kv_at(half, (y + Y - 1) % Y, (z + d) % Z)
            arrived(piece, row_send.at[half, 0, d], row_recv.at[half, 0, d], y_peer(Y - 1))
            if Y > 3 and 2 * d < Z:
                start(piece, piece, row_send.at[half, 2, d], row_recv.at[half, 2, d], y_peer(1))
        if Y > 2:
            piece = kv_at(half, (y + 1) % Y, (z + d) % Z)
            arrived(piece, row_send.at[half, 1, d], row_recv.at[half, 1, d], y_peer(1))
            if Y > 3 and 2 * d >= Z:
                start(
                    piece, piece, row_send.at[half, 2, d], row_recv.at[half, 2, d], y_peer(Y - 1)
                )

    def row_last(half, d):
        if Y > 3:
            piece = kv_at(half, (y + 2) % Y, (z + d) % Z)
            arrived(
                piece,
                row_send.at[half, 2, d],
                row_recv.at[half, 2, d],
                y_peer(Y - 1 if 2 * d < Z else 1),
            )

    def offsets(s):
        found = []
        if s < right_steps:
            found.append(Z - 1 - s)
        if s < left_steps:
            found.append(1 + s)
        return found

    ring_start(0, 0)
    row_start(0, 0)
    start(
        q_ref.at[:, pl.ds(pl.multiple_of((1 - x) * QW, QW), QW)],
        q_far,
        pair_send.at[2],
        pair_recv.at[2],
        partner,
    )

    arrived(tail_x, tail_send.at[0], tail_recv.at[0], before)
    arrived(tail_b, tail_send.at[1], tail_recv.at[1], before)
    arrived(tail_c, tail_send.at[2], tail_recv.at[2], before)
    inside = jnp.where(seq > 0, 1.0, 0.0).astype(F32)

    def conv_silu(pad, tail, rows, weights):
        pad[0:8, :] = tail[8:16, :].astype(F32) * inside
        pad[8 : T + 8, :] = rows.astype(F32)
        total = weights[0:1, :] * pad[5 : T + 5, :]
        for k in range(1, CONV):
            total = total + weights[k : k + 1, :] * pad[5 + k : T + 5 + k, :]
        return silu(total)

    for g in range(G):
        cols = slice(g * STATE, (g + 1) * STATE)
        b_now = conv_silu(pad_s, tail_b[:, cols], b_ref[:, cols], wb_ref[:, cols])
        b_held[g] = b_now.astype(BF16)
        b_turned[g] = b_now.T.astype(BF16)
        c_now = conv_silu(pad_s, tail_c[:, cols], c_ref[:, cols], wc_ref[:, cols])
        c_held[g] = c_now.astype(BF16)

    HALF = W // 2
    chunks = W // 128

    def pack(row):
        parts = [row[:, i * 128 : (i + 1) * 128] for i in range(chunks)]
        if chunks < 8:
            parts.append(jnp.ones((8 - chunks, 128), F32))
        return jnp.concatenate(parts, axis=0)

    def unpack(packed, half):
        return jnp.concatenate(
            [packed[i : i + 1] for i in range(half * chunks // 2, (half + 1) * chunks // 2)], axis=1
        )

    def advance(half, s):
        if s < right_steps:
            ring_wait(half, s)
            if s + 1 < right_steps:
                ring_start(half, s + 1)
            for d in offsets(s):
                row_start(half, d)

    def pair_arrives():
        for i in range(2):
            arrived(
                kv.at[i, pl.ds(pl.multiple_of(block_of(1, y, z) * T, T), T), :],
                pair_send.at[i],
                pair_recv.at[i],
                partner,
            )
        ring_start(1, 0)
        row_start(1, 0)

    def slice_of_heads(d):
        k = (z + d) % Z
        at = pl.ds(pl.multiple_of(k * W, W), W)
        spread = jnp.where(
            lax.broadcasted_iota(jnp.int32, (heads, W), 0)
            == k * (W // P_SIZE) + lax.broadcasted_iota(jnp.int32, (heads, W), 1) // P_SIZE,
            1.0,
            0.0,
        ).astype(BF16)
        per_lane = nn(columns_high, spread) + nn(columns_low, spread)
        per_whole = nn(whole_high, spread) + nn(whole_low, spread)
        now = conv_silu(pad_x, tail_x[:, at], x_ref[:, at], wx_ref[:, at])
        signal[:, at] = now
        scaled[:, at] = (now * per_lane[:T]).astype(BF16)
        entry_decay[:, at] = per_lane[2 * T :]
        skip_rows[:, at] = per_whole[8:]
        weighted = (now * per_lane[T : 2 * T]).astype(BF16)
        state = nn(b_turned[k * W // GW], weighted).astype(BF16)
        packed = pack(per_whole[0:1])
        if d:
            decay_out[d] = packed
            for half in range(2):
                state_out[half, d] = state[:, half * HALF : (half + 1) * HALF]
            start(decay_out.at[d], decay_in.at[z], a2a_send.at[2, d], a2a_recv.at[2, d], z_peer(d))
            start_state(0, d)
        else:
            decay_in[z] = packed
            for half in range(2):
                state_in[half, z] = state[:, half * HALF : (half + 1) * HALF]

    def start_state(half, d):
        start(
            state_out.at[half, d],
            state_in.at[half, z],
            a2a_send.at[half, d],
            a2a_recv.at[half, d],
            z_peer(d),
        )

    todo = [lambda: advance(0, 0), pair_arrives, lambda: advance(1, 0), lambda: advance(0, 1)]
    order = [*range(1, Z), 0]
    for i, d in enumerate(order):
        slice_of_heads(d)
        if i % 2 and todo:
            todo.pop(0)()
    for d in range(1, Z):
        start_state(1, d)
    for act in todo:
        act()

    causal = rows_at >= cols_at
    couplings = [nt(c_held[g], b_held[g]) for g in range(G)]
    lane_at = lax.broadcasted_iota(jnp.int32, (T, 2 * P_SIZE), 1)

    def pair_of_heads(p):
        mixes = []
        for h in (2 * p, 2 * p + 1):
            spread = log_held[:, h : h + 1] - logt_held[h : h + 1, :]
            decays = jnp.exp(jnp.where(causal, spread, LOWEST))
            mixes.append((decays * couplings[h * P_SIZE // GW]).astype(BF16))
        two = scaled[:, p * 128 : (p + 1) * 128]
        zero = jnp.zeros_like(two)
        stacked = jnp.concatenate(
            [jnp.where(lane_at < P_SIZE, two, zero), jnp.where(lane_at < P_SIZE, zero, two)],
            axis=0,
        )
        diagonal[:, p * 128 : (p + 1) * 128] = nn(jnp.concatenate(mixes, axis=1), stacked)

    pairs = heads // 2
    todo = []
    for n in range(1, right_steps):
        todo.append(lambda n=n: advance(1, n))
        if n + 1 < right_steps:
            todo.append(lambda n=n: advance(0, n + 1))
    for p in range(pairs):
        pair_of_heads(p)
        if p % 3 == 2 and todo:
            todo.pop(0)()
    for act in todo:
        act()

    for d in range(1, Z):
        source = (z + Z - d) % Z
        arrived(decay_in.at[source], a2a_send.at[2, d], a2a_recv.at[2, d], z_peer(Z - d))
    running_decay = jnp.ones((8, 128), F32)
    for i in range(Z):
        running_decay = running_decay * decay_in[i]
    total_decay_out[...] = running_decay
    total_decay_in[group] = running_decay
    for d in range(1, 2 * Y):
        start(
            total_decay_out,
            total_decay_in.at[group],
            tot_send.at[2, d],
            tot_recv.at[2, d],
            group_peer(d),
        )

    def scan(half):
        for d in range(1, Z):
            source = (z + Z - d) % Z
            arrived(
                state_in.at[half, source], a2a_send.at[half, d], a2a_recv.at[half, d], z_peer(Z - d)
            )
        running = jnp.zeros((STATE, HALF), F32)
        for i in range(Z):
            prefix[half, i] = running
            running = running * unpack(decay_in[i], half) + state_in[half, i].astype(F32)
        total_out[half] = running.astype(BF16)
        total_in[half, group] = running.astype(BF16)
        for d in range(1, 2 * Y):
            start(
                total_out.at[half],
                total_in.at[half, group],
                tot_send.at[half, d],
                tot_recv.at[half, d],
                group_peer(d),
            )

    def enter(half):
        for d in range(1, 2 * Y):
            source = (group + 2 * Y - d) % (2 * Y)
            back = group_peer(2 * Y - d)
            if half == 0:
                arrived(total_decay_in.at[source], tot_send.at[2, d], tot_recv.at[2, d], back)
            arrived(total_in.at[half, source], tot_send.at[half, d], tot_recv.at[half, d], back)
        entering = jnp.zeros((STATE, HALF), F32)
        for i in range(2 * Y):
            further = entering * unpack(total_decay_in[i], half) + total_in[half, i].astype(F32)
            entering = jnp.where(i < group, further, entering)
        so_far = jnp.ones((8, 128), F32)
        for i in range(Z):
            enter_out[half, i] = (prefix[half, i] + entering * unpack(so_far, half)).astype(BF16)
            so_far = so_far * decay_in[i]
        for d in range(1, Z):
            k = (z + d) % Z
            start(
                enter_out.at[half, k],
                enter_in.at[half, z],
                back_send.at[half, d],
                back_recv.at[half, d],
                z_peer(d),
            )
        enter_in[half, z] = enter_out[half, z]

    piece_order = [0]
    for n in range(right_steps):
        piece_order += offsets(n)
    scale = math.log2(math.e) / math.sqrt(HD)
    all_rows = grouped * T
    chunk = min(ROWS, all_rows)

    key_tile = min(KEY_TILE, Z * T)
    m_held[...] = jnp.full(m_held.shape, LOWEST, F32)
    acc_held[...] = jnp.zeros(acc_held.shape, F32)

    def tile(which, start_key, position, masked):
        keys_at = pl.ds(pl.multiple_of(start_key, key_tile), key_tile)
        keys = kv[0, keys_at, :]
        values = jnp.concatenate([kv[1, keys_at, :], jnp.ones((key_tile, HD), BF16)], axis=1)
        for r in range(0, all_rows, chunk):
            scores = nt(q_rows[which, r : r + chunk, :], keys)
            if masked:
                row = lax.broadcasted_iota(jnp.int32, (chunk, key_tile), 0) % T
                col = lax.broadcasted_iota(jnp.int32, (chunk, key_tile), 1)
                scores = jnp.where(col + start_key <= row + position * T, scores, LOWEST)
            old = m_held[which, r : r + chunk, :]
            new = jnp.maximum(old, jnp.max(scores, axis=1, keepdims=True))
            m_held[which, r : r + chunk, :] = new
            factor = jnp.exp2((old - new) * scale)
            weights = jnp.concatenate(
                [
                    jnp.exp2((scores[:, j : j + HD] - new) * scale).astype(BF16)
                    for j in range(0, key_tile, HD)
                ],
                axis=1,
            )
            product = nn(weights, values)
            acc_held[which, r : r + chunk, :] = (
                acc_held[which, r : r + chunk, :] * jnp.concatenate([factor, factor], axis=1)
                + product
            )

    def attend(rows):
        def one(i, carry):
            which, half, at = i // 2 % 2, i % 2, i // 4
            yy = rows[0] if len(rows) == 1 else rows[0] * (1 - at) + rows[1] * at
            position = (1 - which) * seq + which * block_of(1, y, z)
            first = (1 - half) * block_of(0, yy, 0) + half * block_of(1, yy, 0)
            inside_row = jnp.minimum(jnp.maximum(position - first, 0), Z)
            full = inside_row * T // key_tile

            def body(n, c):
                tile(which, first * T + n * key_tile, position, False)
                return c

            lax.fori_loop(0, full, body, 0)

            @pl.when((position >= first) & (position < first + Z))
            def _():
                tile(which, first * T + full * key_tile, position, True)

            return carry

        lax.fori_loop(0, 4 * len(rows), one, 0)

    scan(0)
    scan(1)
    arrived(q_far, pair_send.at[2], pair_recv.at[2], partner)
    for h in range(grouped):
        q_rows[1, h * T : (h + 1) * T, :] = q_far[:, h * HD : (h + 1) * HD]
    for d in piece_order[: Z // 2]:
        for half in range(2):
            row_forward(half, d)
    attend([y])
    enter(0)
    for d in piece_order[Z // 2 :]:
        for half in range(2):
            row_forward(half, d)
    enter(1)
    if Y == 2:
        attend([(y + 1) % Y])
    if Y > 2:
        attend([(y + Y - 1) % Y, (y + 1) % Y])
    for d in range(Z):
        for half in range(2):
            row_last(half, d)
    if Y > 3:
        attend([(y + 2) % Y])

    def result(which, h):
        both = acc_held[which, h * T : (h + 1) * T, :]
        return (both[:, :HD] / both[:, HD:]).astype(BF16)

    for h in range(grouped):
        o_far[:, h * HD : (h + 1) * HD] = result(1, h)
    start(o_far, o_in, pair_send.at[3], pair_recv.at[3], partner)
    for h in range(grouped):
        attn_ref[:, pl.ds(pl.multiple_of(x * QW + h * HD, HD), HD)] = result(0, h)

    for d in range(1, Z):
        source = (z + Z - d) % Z
        for half in range(2):
            arrived(
                enter_in.at[half, source], back_send.at[half, d], back_recv.at[half, d], z_peer(Z - d)
            )
    summed = jnp.zeros((T, 128), F32)
    for k in range(Z):
        cols = slice(k * W, (k + 1) * W)
        entry = jnp.concatenate([enter_in[0, k], enter_in[1, k]], axis=1)
        off = nn(c_held[k * W // GW], entry)
        mixed = diagonal[:, cols] + entry_decay[:, cols] * off
        mixed = mixed + skip_rows[0:1, cols] * signal[:, cols]
        now = mixed * silu(gate_ref[:, cols].astype(F32))
        gated[:, cols] = now
        now = now * now
        for j in range(0, W, 128):
            summed = summed + now[:, j : j + 128]
    squares[t] = nt(jnp.ones((8, 128), F32), summed, HIGHEST)
    for d in range(1, TP):
        start(squares.at[t], squares.at[t], sq_send.at[d], sq_recv.at[d], tp_peer(d))
    for d in range(1, TP):
        source = (t + TP - d) % TP
        arrived(squares.at[source], sq_send.at[d], sq_recv.at[d], tp_peer(TP - d))
    everything = squares[0]
    for i in range(1, TP):
        everything = everything + squares[i]
    everything = jnp.broadcast_to(everything[0:1, :], (T, T)).T
    factor = lax.rsqrt(everything / (HW * TP) + EPSILON)
    for j in range(0, HW, 128):
        mixer_ref[:, j : j + 128] = (
            gated[:, j : j + 128] * factor * gain_ref[:, j : j + 128]
        ).astype(BF16)

    arrived(o_in, pair_send.at[3], pair_recv.at[3], partner)
    attn_ref[:, pl.ds(pl.multiple_of((1 - x) * QW, QW), QW)] = o_in[...]
    for copy in sent:
        copy.wait_send()


def shards(dims, *args):
    (x, gate, b, c, step, bias, rate, skip, wx, wb, wc, gain, q, k, v) = args
    bias, rate, skip, gain = (a.reshape(1, -1) for a in (bias, rate, skip, gain))
    Y, Z, TP = dims
    T, HW = x.shape
    W = HW // Z
    G = b.shape[1] // STATE
    count = 2 * Y * Z
    QW = q.shape[1] // 2
    rows = QW // HD * T
    vmem, dma = pltpu.VMEM, pltpu.SemaphoreType.DMA
    scratch = [
        vmem((TAIL, HW), BF16),
        vmem((TAIL, G * STATE), BF16),
        vmem((TAIL, G * STATE), BF16),
        vmem((T + 8, W), F32),
        vmem((T + 8, STATE), F32),
        vmem((T, HW), F32),
        vmem((T, HW), BF16),
        vmem((T, HW), F32),
        vmem((8, HW), F32),
        vmem((G, STATE, T), BF16),
        vmem((G, T, STATE), BF16),
        vmem((G, T, STATE), BF16),
        vmem((T, STATE), F32),
        vmem((STATE, T), F32),
        vmem((2, Z, STATE, W // 2), BF16),
        vmem((Z, 8, 128), F32),
        vmem((2, Z, STATE, W // 2), BF16),
        vmem((Z, 8, 128), F32),
        vmem((2, Z, STATE, W // 2), F32),
        vmem((2, STATE, W // 2), BF16),
        vmem((8, 128), F32),
        vmem((2, 2 * Y, STATE, W // 2), BF16),
        vmem((2 * Y, 8, 128), F32),
        vmem((2, Z, STATE, W // 2), BF16),
        vmem((2, Z, STATE, W // 2), BF16),
        vmem((T, HW), F32),
        vmem((T, HW), F32),
        vmem((TP, 8, 128), F32),
        vmem((2, count * T, HD), BF16),
        vmem((T, QW), BF16),
        vmem((2, rows, HD), BF16),
        vmem((T, QW), BF16),
        vmem((T, QW), BF16),
        vmem((2, rows, HD), F32),
        vmem((2, rows, 2 * HD), F32),
        dma((3,)),
        dma((3,)),
        dma((4,)),
        dma((4,)),
        dma((2, 2, max(Z // 2, 1))),
        dma((2, 2, max(Z // 2, 1))),
        dma((2, 3, Z)),
        dma((2, 3, Z)),
        dma((3, Z)),
        dma((3, Z)),
        dma((3, 2 * Y)),
        dma((3, 2 * Y)),
        dma((2, Z)),
        dma((2, Z)),
        dma((TP,)),
        dma((TP,)),
    ]
    whole = pl.BlockSpec(memory_space=pltpu.VMEM)
    return pl.pallas_call(
        functools.partial(kernel, dims),
        out_shape=(
            jax.ShapeDtypeStruct((T, HW), BF16),
            jax.ShapeDtypeStruct((T, 2 * QW), BF16),
        ),
        in_specs=[whole] * 15,
        out_specs=(whole, whole),
        scratch_shapes=scratch,
        compiler_params=pltpu.CompilerParams(
            collective_id=0, has_side_effects=True, vmem_limit_bytes=60 * 1024 * 1024
        ),
        name="hybrid",
    )(x, gate, b, c, step.T, bias, rate, skip, wx, wb, wc, gain, q, k, v)


def build(mesh, Y, Z):
    TP = mesh.shape["tp"]
    torus = Mesh(mesh.devices.reshape(2, Y, Z, TP), (*SEQ, "tp"))
    cut, by_tp = P(SEQ, "tp"), P("tp")
    taps = P(None, "tp")
    placed = (cut,) * 5 + (by_tp,) * 3 + (taps,) * 3 + (by_tp,) + (cut,) * 3
    return jax.shard_map(
        functools.partial(shards, (Y, Z, TP)),
        mesh=torus,
        in_specs=placed,
        out_specs=(cut, cut),
        check_vma=False,
    )


def solution(mesh):
    return build(mesh, 4, 8)
```

```python
import functools
import math

import jax
import jax.numpy as jnp
from jax import lax
from jax.experimental import pallas as pl
from jax.experimental.pallas import tpu as pltpu
from jax.sharding import Mesh
from jax.sharding import PartitionSpec as P

P_SIZE = 64
STATE = 128
HD = 128
CONV = 4
SEQ = ("seq_0", "seq_1", "seq_2")
MESH = pl.DeviceIdType.MESH
F32 = jnp.float32
BF16 = jnp.bfloat16
HIGHEST = lax.Precision.HIGHEST
EPSILON = 1e-05
LOWEST = -1e30
KEY_TILE = 512
ROWS = 256
TAIL = 16


def nt(a, b, precision=None):
    return lax.dot_general(
        a, b, (((1,), (1,)), ((), ())), preferred_element_type=F32, precision=precision
    )


def nn(a, b, precision=None):
    return lax.dot_general(
        a, b, (((1,), (0,)), ((), ())), preferred_element_type=F32, precision=precision
    )


def silu(a):
    return a / (1.0 + jnp.exp(-a))


def two_parts(value):
    high = value.astype(BF16)
    low = (value - high.astype(F32)).astype(BF16)
    return high, low


def kernel(
    dims,
    x_far,
    gate_far,
    b_far,
    c_far,
    step_ref,
    bias_ref,
    rate_ref,
    skip_ref,
    wx_ref,
    wb_ref,
    wc_ref,
    gain_ref,
    q_far_in,
    k_far,
    v_far,
    mixer_ref,
    attn_ref,
    x_ref,
    gate_ref,
    b_ref,
    c_ref,
    q_ref,
    k_ref,
    v_ref,
    load_sems,
    tail_x,
    tail_b,
    tail_c,
    pad_x,
    pad_s,
    b_first,
    c_first,
    weighted,
    early_step,
    early_close,
    whole_decay,
    signal,
    scaled,
    entry_decay,
    skip_rows,
    b_turned,
    b_held,
    c_held,
    log_held,
    logt_held,
    state_out,
    decay_out,
    state_in,
    decay_in,
    prefix,
    total_out,
    total_decay_out,
    total_in,
    total_decay_in,
    enter_out,
    enter_in,
    diagonal,
    gated,
    squares,
    kv,
    q_far,
    q_rows,
    o_far,
    o_in,
    m_held,
    acc_held,
    tail_send,
    tail_recv,
    pair_send,
    pair_recv,
    ring_send,
    ring_recv,
    row_send,
    row_recv,
    a2a_send,
    a2a_recv,
    tot_send,
    tot_recv,
    back_send,
    back_recv,
    sq_send,
    sq_recv,
):
    Y, Z, TP = dims
    T = x_ref.shape[0]
    HW = x_ref.shape[1]
    heads = HW // P_SIZE
    W = HW // Z
    G = b_ref.shape[1] // STATE
    GW = HW // G
    YZ = Y * Z
    QW = q_ref.shape[1] // 2
    grouped = QW // HD

    x = lax.axis_index("seq_0")
    y = lax.axis_index("seq_1")
    z = lax.axis_index("seq_2")
    t = lax.axis_index("tp")
    seq = x * YZ + y * Z + z
    count = 2 * YZ

    def place(index):
        return (index // YZ, (index // Z) % Y, index % Z, t)

    after = place((seq + 1) % count)
    before = place((seq + count - 1) % count)

    core = t % 2
    high = y // (Y // 2)
    own_slot = (core + high) % 2 == 0
    facing = Y - 1 - y
    beside = y + 1 - 2 * (y % 2)
    sibling = (x, y, z, t + 1 - 2 * core)

    def z_peer(d):
        return (x, y, (z + d) % Z, t)

    y_peer = (x, beside, z, t)

    group = x * Y + y

    def group_peer(d):
        other = (group + d) % (2 * Y)
        return (other // Y, other % Y, z, t)

    def tp_peer(d):
        return (x, y, z, (t + d) % TP)

    total_in[...] = jnp.zeros(total_in.shape, BF16)
    total_decay_in[...] = jnp.ones(total_decay_in.shape, F32)
    barrier = pltpu.get_barrier_semaphore()
    greeted = [after, before]
    greeted += [z_peer(d) for d in range(1, Z)]
    greeted += [group_peer(d) for d in range(1, 2 * Y)]
    greeted += [tp_peer(d) for d in range(1, TP)]
    greeted += [(1 - x, y, z, t + 1 - 2 * core), (x, facing, z, t + 1 - 2 * core)]
    for peer in greeted:
        pl.semaphore_signal(barrier, inc=1, device_id=peer, device_id_type=MESH)

    def remote(src, dst, send, recv, peer):
        return pltpu.make_async_remote_copy(
            src_ref=src,
            dst_ref=dst,
            send_sem=send,
            recv_sem=recv,
            device_id=peer,
            device_id_type=MESH,
        )

    sent = []
    inside = jnp.where(seq > 0, 1.0, 0.0).astype(F32)
    far = (x_far, b_far, c_far, k_far, v_far, q_far_in, gate_far)
    held = (x_ref, b_ref, c_ref, k_ref, v_ref, q_ref, gate_ref)
    loads = [
        pltpu.make_async_copy(src, dst, load_sems.at[i]) for i, (src, dst) in enumerate(zip(far, held))
    ]
    for load in loads:
        load.start()

    def start(src, dst, send, recv, peer):
        copy = remote(src, dst, send, recv, peer)
        copy.start()
        sent.append(copy)

    def arrived(dst, send, recv, peer):
        remote(dst, dst, send, recv, peer).wait_recv()

    def block_of(slot, sharer, other, zz):
        xx = (x + core + sharer + high + slot) % 2
        low = facing * high + y * (1 - high)
        low = low * (1 - other) + (Y // 2 - 1 - low) * other
        up = (high + slot) % 2
        return xx * YZ + (low * (1 - up) + (Y - 1 - low) * up) * Z + zz

    def kv_at(slot, sharer, other, zz):
        first = pl.multiple_of(block_of(slot, sharer, other, zz) * T, T)
        return kv.at[:, pl.ds(first, T), :]

    own_rows = pl.ds(pl.multiple_of(seq * T, T), T)

    turned = jnp.concatenate(
        [step_ref[...], jnp.zeros((STATE - heads, T), F32)], axis=0
    ).T
    step_in = turned[:, :heads] + bias_ref[...]
    step = jnp.maximum(step_in, 0.0) + jnp.log(1.0 + jnp.exp(-jnp.abs(step_in)))
    rows_at = lax.broadcasted_iota(jnp.int32, (T, T), 0)
    cols_at = lax.broadcasted_iota(jnp.int32, (T, T), 1)
    lower = jnp.where(rows_at >= cols_at, 1.0, 0.0).astype(F32)
    wide = jnp.concatenate(
        [-step * rate_ref[...], jnp.zeros((T, STATE - heads), F32)], axis=1
    )
    log_decay = nn(lower, wide, HIGHEST)
    log_held[...] = log_decay
    logt_held[...] = log_decay.T
    log_decay = log_decay[:, :heads]
    last = log_decay[T - 1 : T, :]
    closing = jnp.exp(last - log_decay)
    columns = jnp.concatenate([step, step * closing, jnp.exp(log_decay)], axis=0)
    columns_high, columns_low = two_parts(columns)
    whole = jnp.concatenate(
        [
            jnp.broadcast_to(jnp.exp(last), (8, heads)),
            jnp.broadcast_to(skip_ref[...], (8, heads)),
        ],
        axis=0,
    )
    whole_high, whole_low = two_parts(whole)

    def conv_silu(pad, tail, rows, weights):
        count = rows.shape[0]
        if tail is None:
            pad[0:8, :] = jnp.zeros((8, rows.shape[1]), F32)
        else:
            pad[0:8, :] = tail[8:16, :].astype(F32) * inside
        pad[8 : count + 8, :] = rows.astype(F32)
        total = weights[0:1, :] * pad[5 : count + 5, :]
        for k in range(1, CONV):
            total = total + weights[k : k + 1, :] * pad[5 + k : count + 5 + k, :]
        return silu(total)

    for load in loads[:-1]:
        load.wait()

    @pl.when(own_slot)
    def _():
        kv[0, own_rows, :] = k_ref[:, pl.ds(pl.multiple_of(x * HD, HD), HD)]
        kv[1, own_rows, :] = v_ref[:, pl.ds(pl.multiple_of(x * HD, HD), HD)]
        for h in range(grouped):
            q_rows[0, h * T : (h + 1) * T, :] = q_ref[
                :, pl.ds(pl.multiple_of(x * QW + h * HD, HD), HD)
            ]

    pl.semaphore_wait(barrier, len(greeted))

    start(x_ref.at[T - TAIL :, :], tail_x, tail_send.at[0], tail_recv.at[0], after)
    start(b_ref.at[T - TAIL :, :], tail_b, tail_send.at[1], tail_recv.at[1], after)
    start(c_ref.at[T - TAIL :, :], tail_c, tail_send.at[2], tail_recv.at[2], after)
    across = (1 - x, y, z, t + 1 - 2 * core)
    face = (x, facing, z, t + 1 - 2 * core)
    corner = (1 - x, facing, z, t)

    def kv_columns(j):
        return pl.ds(pl.multiple_of(j * HD, HD), HD)

    def q_columns(j):
        return pl.ds(pl.multiple_of(j * QW, QW), QW)

    def pair_copies(what):
        found = []
        for condition, j, slot, peer in (
            (own_slot, 1 - x, 0, across),
            (~own_slot, x, 1, face),
            (~own_slot, 1 - x, 1, corner),
        ):
            n = len(found)
            if what == 2:
                copy = remote(
                    q_ref.at[:, q_columns(j)], q_far.at[slot], pair_send.at[2, n],
                    pair_recv.at[2, slot], peer,
                )
            else:
                copy = remote(
                    (k_ref, v_ref)[what].at[:, kv_columns(j)], kv.at[what, own_rows, :],
                    pair_send.at[what, n], pair_recv.at[what, slot], peer,
                )
            found.append((condition, copy))
        return found

    def back_copies():
        found = []
        for condition, slot, peer in (
            (~own_slot, 0, across),
            (~own_slot, 1, face),
            (own_slot, 1, corner),
        ):
            found.append(
                (
                    condition,
                    remote(
                        o_far.at[slot], o_in.at[x], pair_send.at[3, len(found)],
                        pair_recv.at[3, x], peer,
                    ),
                )
            )
        return found

    def start_all(pieces):
        for condition, copy in pieces:
            pl.when(condition)(copy.start)

    quad = [pair_copies(0), pair_copies(1)]
    for pieces in quad:
        start_all(pieces)

    right_steps = Z // 2
    left_steps = (Z - 1) // 2

    def ring_start(slot, s):
        if s < right_steps:
            piece = kv_at(slot, 0, 0, (z + Z - s) % Z)
            start(piece, piece, ring_send.at[slot, 0, s], ring_recv.at[slot, 0, s], z_peer(1))
        if s < left_steps:
            piece = kv_at(slot, 0, 0, (z + s) % Z)
            start(piece, piece, ring_send.at[slot, 1, s], ring_recv.at[slot, 1, s], z_peer(Z - 1))

    def ring_wait(slot, s):
        if s < right_steps:
            piece = kv_at(slot, 0, 0, (z + Z - 1 - s) % Z)
            arrived(piece, ring_send.at[slot, 0, s], ring_recv.at[slot, 0, s], z_peer(Z - 1))
        if s < left_steps:
            piece = kv_at(slot, 0, 0, (z + 1 + s) % Z)
            arrived(piece, ring_send.at[slot, 1, s], ring_recv.at[slot, 1, s], z_peer(1))

    def row_start(slot, d):
        piece = kv_at(slot, 0, 0, (z + d) % Z)
        start(piece, piece, row_send.at[slot, 0, d], row_recv.at[slot, 0, d], y_peer)
        start(piece, piece, row_send.at[slot, 1, d], row_recv.at[slot, 1, d], sibling)

    def near_arrives(slot, d):
        piece = kv_at(slot, 1, 0, (z + d) % Z)
        arrived(piece, row_send.at[slot, 1, d], row_recv.at[slot, 1, d], sibling)

    def row_forward(slot, d):
        piece = kv_at(slot, 0, 1, (z + d) % Z)
        arrived(piece, row_send.at[slot, 0, d], row_recv.at[slot, 0, d], y_peer)
        start(piece, piece, row_send.at[slot, 2, d], row_recv.at[slot, 2, d], sibling)

    def row_last(slot, d):
        piece = kv_at(slot, 1, 1, (z + d) % Z)
        arrived(piece, row_send.at[slot, 2, d], row_recv.at[slot, 2, d], sibling)

    def offsets(s):
        found = []
        if s < right_steps:
            found.append(Z - 1 - s)
        if s < left_steps:
            found.append(1 + s)
        return found

    quad.append(pair_copies(2))
    start_all(quad[2])

    def pair_arrives(slot):
        def wait():
            for i in range(2):
                place = block_of(slot, 0, 0, z)
                arrived(
                    kv.at[i, pl.ds(pl.multiple_of(place * T, T), T), :],
                    pair_send.at[i, 0],
                    pair_recv.at[i, slot],
                    across,
                )

        if slot == 0:
            pl.when(~own_slot)(wait)
        else:
            wait()
        ring_start(slot, 0)
        row_start(slot, 0)

    b_first[...] = conv_silu(pad_s, None, b_ref[...], wb_ref)
    c_first[...] = conv_silu(pad_s, None, c_ref[...], wc_ref)
    for k in range(Z):
        at = slice(k * W, (k + 1) * W)
        spread = jnp.where(
            lax.broadcasted_iota(jnp.int32, (heads, W), 0)
            == k * (W // P_SIZE) + lax.broadcasted_iota(jnp.int32, (heads, W), 1) // P_SIZE,
            1.0,
            0.0,
        ).astype(BF16)
        per_lane = nn(columns_high, spread) + nn(columns_low, spread)
        per_whole = nn(whole_high, spread) + nn(whole_low, spread)
        now = conv_silu(pad_x, None, x_ref[:, at], wx_ref[:, at])
        signal[:, at] = now
        scaled[:, at] = (now * per_lane[:T]).astype(BF16)
        weighted[:, at] = (now * per_lane[T : 2 * T]).astype(BF16)
        early_step[:, at] = per_lane[:TAIL]
        early_close[:, at] = per_lane[T : T + TAIL]
        entry_decay[:, at] = per_lane[2 * T :]
        skip_rows[:, at] = per_whole[8:]
        whole_decay[:, at] = per_whole[:8]


    arrived(tail_x, tail_send.at[0], tail_recv.at[0], before)
    arrived(tail_b, tail_send.at[1], tail_recv.at[1], before)
    arrived(tail_c, tail_send.at[2], tail_recv.at[2], before)
    b_first[:TAIL, :] = conv_silu(pad_s, tail_b, b_ref[:TAIL, :], wb_ref)
    c_first[:TAIL, :] = conv_silu(pad_s, tail_c, c_ref[:TAIL, :], wc_ref)
    for g in range(G):
        cols = slice(g * STATE, (g + 1) * STATE)
        b_held[g] = b_first[:, cols].astype(BF16)
        b_turned[g] = b_first[:, cols].T.astype(BF16)
        c_held[g] = c_first[:, cols].astype(BF16)
    for k in range(Z):
        at = slice(k * W, (k + 1) * W)
        now = conv_silu(pad_x, tail_x[:, at], x_ref[:TAIL, at], wx_ref[:, at])
        signal[:TAIL, at] = now
        scaled[:TAIL, at] = (now * early_step[:, at]).astype(BF16)
        weighted[:TAIL, at] = (now * early_close[:, at]).astype(BF16)
    pair_arrives(0)
    pair_arrives(1)

    HALF = W // 2
    chunks = W // 128

    def pack(row):
        parts = [row[:, i * 128 : (i + 1) * 128] for i in range(chunks)]
        if chunks < 8:
            parts.append(jnp.ones((8 - chunks, 128), F32))
        return jnp.concatenate(parts, axis=0)

    def unpack(packed, half):
        return jnp.concatenate(
            [packed[i : i + 1] for i in range(half * chunks // 2, (half + 1) * chunks // 2)], axis=1
        )

    def advance(half, s):
        if s < right_steps:
            ring_wait(half, s)
            if s + 1 < right_steps:
                ring_start(half, s + 1)
            for d in offsets(s):
                row_start(half, d)

    def slice_of_heads(d):
        k = (z + d) % Z
        at = pl.ds(pl.multiple_of(k * W, W), W)
        state = nn(b_turned[k * W // GW], weighted[:, at]).astype(BF16)
        packed = pack(whole_decay[0:1, at])
        if d:
            decay_out[d] = packed
            for half in range(2):
                state_out[half, d] = state[:, half * HALF : (half + 1) * HALF]
            start(decay_out.at[d], decay_in.at[z], a2a_send.at[2, d], a2a_recv.at[2, d], z_peer(d))
        else:
            decay_in[z] = packed
            for half in range(2):
                state_in[half, z] = state[:, half * HALF : (half + 1) * HALF]

    def start_state(half, d):
        start(
            state_out.at[half, d],
            state_in.at[half, z],
            a2a_send.at[half, d],
            a2a_recv.at[half, d],
            z_peer(d),
        )

    for d in [*range(1, Z), 0]:
        slice_of_heads(d)

    causal = rows_at >= cols_at
    couplings = [nt(c_held[g], b_held[g]) for g in range(G)]
    lane_at = lax.broadcasted_iota(jnp.int32, (T, 2 * P_SIZE), 1)

    def pair_of_heads(p):
        mixes = []
        for h in (2 * p, 2 * p + 1):
            spread = log_held[:, h : h + 1] - logt_held[h : h + 1, :]
            decays = jnp.exp(jnp.where(causal, spread, LOWEST))
            mixes.append((decays * couplings[h * P_SIZE // GW]).astype(BF16))
        two = scaled[:, p * 128 : (p + 1) * 128]
        zero = jnp.zeros_like(two)
        stacked = jnp.concatenate(
            [jnp.where(lane_at < P_SIZE, two, zero), jnp.where(lane_at < P_SIZE, zero, two)],
            axis=0,
        )
        diagonal[:, p * 128 : (p + 1) * 128] = nn(jnp.concatenate(mixes, axis=1), stacked)

    pairs = heads // 2

    def some_pairs(low, high):
        for p in range(low * pairs // 16, high * pairs // 16):
            pair_of_heads(p)

    def ring_step(s):
        for slot in range(2):
            advance(slot, s)

    for d in range(1, Z):
        source = (z + Z - d) % Z
        arrived(decay_in.at[source], a2a_send.at[2, d], a2a_recv.at[2, d], z_peer(Z - d))
    running_decay = jnp.ones((8, 128), F32)
    for i in range(Z):
        running_decay = running_decay * decay_in[i]
    total_decay_out[...] = running_decay
    total_decay_in[group] = running_decay
    totals_sent = []

    def total_start(src, dst, kind, d):
        copy = remote(src, dst, tot_send.at[kind, d], tot_recv.at[kind, d], group_peer(d))
        later = group + d < 2 * Y
        pl.when(later)(copy.start)
        totals_sent.append((later, copy))

    def total_arrived(dst, kind, d):
        @pl.when(group >= d)
        def _():
            arrived(dst, tot_send.at[kind, d], tot_recv.at[kind, d], group_peer(2 * Y - d))

    for d in range(1, 2 * Y):
        total_start(total_decay_out, total_decay_in.at[group], 2, d)

    def scan(half):
        for d in range(1, Z):
            source = (z + Z - d) % Z
            arrived(
                state_in.at[half, source], a2a_send.at[half, d], a2a_recv.at[half, d], z_peer(Z - d)
            )
        running = jnp.zeros((STATE, HALF), F32)
        for i in range(Z):
            prefix[half, i] = running
            running = running * unpack(decay_in[i], half) + state_in[half, i].astype(F32)
        total_out[half] = running.astype(BF16)
        total_in[half, group] = running.astype(BF16)
        for d in range(1, 2 * Y):
            total_start(total_out.at[half], total_in.at[half, group], half, d)

    def enter(half):
        for d in range(1, 2 * Y):
            source = (group + 2 * Y - d) % (2 * Y)
            if half == 0:
                total_arrived(total_decay_in.at[source], 2, d)
            total_arrived(total_in.at[half, source], half, d)
        entering = jnp.zeros((STATE, HALF), F32)
        for i in range(2 * Y):
            further = entering * unpack(total_decay_in[i], half) + total_in[half, i].astype(F32)
            entering = jnp.where(i < group, further, entering)
        so_far = jnp.ones((8, 128), F32)
        for i in range(Z):
            enter_out[half, i] = (prefix[half, i] + entering * unpack(so_far, half)).astype(BF16)
            so_far = so_far * decay_in[i]
        for d in range(1, Z):
            k = (z + d) % Z
            start(
                enter_out.at[half, k],
                enter_in.at[half, z],
                back_send.at[half, d],
                back_recv.at[half, d],
                z_peer(d),
            )
        enter_in[half, z] = enter_out[half, z]

    piece_order = [0]
    for n in range(right_steps):
        piece_order += offsets(n)
    scale = math.log2(math.e) / math.sqrt(HD)
    all_rows = grouped * T
    chunk = min(ROWS, all_rows)

    span = max(Z // 2, 1)
    key_tile = span * T
    m_held[...] = jnp.full(m_held.shape, LOWEST, F32)
    acc_held[...] = jnp.zeros(acc_held.shape, F32)

    def tile(which, start_key, position, masked):
        keys_at = pl.ds(pl.multiple_of(start_key, key_tile), key_tile)
        keys = kv[0, keys_at, :]
        values = jnp.concatenate([kv[1, keys_at, :], jnp.ones((key_tile, HD), BF16)], axis=1)
        for r in range(0, all_rows, chunk):
            scores = nt(q_rows[which, r : r + chunk, :], keys)
            if masked:
                row = lax.broadcasted_iota(jnp.int32, (chunk, key_tile), 0) % T
                col = lax.broadcasted_iota(jnp.int32, (chunk, key_tile), 1)
                scores = jnp.where(col + start_key <= row + position * T, scores, LOWEST)
            old = m_held[which, r : r + chunk, :]
            new = jnp.maximum(old, jnp.max(scores, axis=1, keepdims=True))
            m_held[which, r : r + chunk, :] = new
            factor = jnp.exp2((old - new) * scale)
            weights = jnp.concatenate(
                [
                    jnp.exp2((scores[:, j : j + HD] - new) * scale).astype(BF16)
                    for j in range(0, key_tile, HD)
                ],
                axis=1,
            )
            product = nn(weights, values)
            acc_held[which, r : r + chunk, :] = (
                acc_held[which, r : r + chunk, :] * jnp.concatenate([factor, factor], axis=1)
                + product
            )

    def attend(other, which, parts):
        near = z // span

        def one(i, carry):
            n = (near + parts[0] + i // 4) % 2
            sharer, slot = i // 2 % 2, i % 2
            position = block_of(which, 0, 0, z)
            first = block_of(slot, sharer, other, 0) + n * span

            @pl.when(first + span <= position)
            def _():
                tile(which, first * T, position, False)

            @pl.when((first <= position) & (position < first + span))
            def _():
                tile(which, first * T, position, True)

            return carry

        lax.fori_loop(0, 4 * len(parts), one, 0)

    def unroll_queries(slot):
        arrived(q_far.at[slot], pair_send.at[2, 0], pair_recv.at[2, slot], across)
        for h in range(grouped):
            q_rows[slot, h * T : (h + 1) * T, :] = q_far[slot, :, h * HD : (h + 1) * HD]

    def result(which, h):
        both = acc_held[which, h * T : (h + 1) * T, :]
        return (both[:, :HD] / both[:, HD:]).astype(BF16)

    def results_leave(slot):
        for h in range(grouped):
            o_far[slot, :, h * HD : (h + 1) * HD] = result(slot, h)
        start_all(returned[slot])

    returned = back_copies()
    returned = [returned[:1], returned[1:]]

    def forward(pieces):
        for d in pieces:
            for slot in range(2):
                row_forward(slot, d)

    far_first = sorted(range(1, Z), key=lambda d: -min(d, Z - d))
    first, second = far_first[: Z // 2], far_first[Z // 2 :]

    def states(half, which):
        for d in which:
            start_state(half, d)

    def near(pieces):
        for d in pieces:
            for slot in range(2):
                near_arrives(slot, d)

    some_pairs(0, 8)
    ring_step(0)
    states(0, first)
    ring_step(1)
    states(0, second)
    ring_step(2)
    some_pairs(8, 16)
    states(1, first)
    states(1, second)
    pl.when(~own_slot)(lambda: unroll_queries(0))
    unroll_queries(1)
    near([d for d in piece_order if d != Z // 2])
    attend(0, 1, (0,))
    ring_step(3)
    near([Z // 2])
    attend(0, 0, (0,))
    scan(0)
    attend(0, 1, (1,))
    scan(1)
    attend(0, 0, (1,))
    enter(0)
    forward(piece_order)
    for d in piece_order:
        for slot in range(2):
            row_last(slot, d)
    enter(1)
    attend(1, 1, (0, 1))
    results_leave(1)
    attend(1, 0, (0, 1))
    results_leave(0)

    @pl.when(own_slot)
    def _():
        attn_ref[:, q_columns(x)] = o_far[0]

    for d in range(1, Z):
        source = (z + Z - d) % Z
        for half in range(2):
            arrived(
                enter_in.at[half, source], back_send.at[half, d], back_recv.at[half, d], z_peer(Z - d)
            )
    loads[-1].wait()
    summed = jnp.zeros((T, 128), F32)
    for k in range(Z):
        cols = slice(k * W, (k + 1) * W)
        entry = jnp.concatenate([enter_in[0, k], enter_in[1, k]], axis=1)
        off = nn(c_held[k * W // GW], entry)
        mixed = diagonal[:, cols] + entry_decay[:, cols] * off
        mixed = mixed + skip_rows[0:1, cols] * signal[:, cols]
        now = mixed * silu(gate_ref[:, cols].astype(F32))
        gated[:, cols] = now
        now = now * now
        for j in range(0, W, 128):
            summed = summed + now[:, j : j + 128]
    squares[t] = nt(jnp.ones((8, 128), F32), summed, HIGHEST)
    for d in range(1, TP):
        start(squares.at[t], squares.at[t], sq_send.at[d], sq_recv.at[d], tp_peer(d))
    for d in range(1, TP):
        source = (t + TP - d) % TP
        arrived(squares.at[source], sq_send.at[d], sq_recv.at[d], tp_peer(TP - d))
    everything = squares[0]
    for i in range(1, TP):
        everything = everything + squares[i]
    everything = jnp.broadcast_to(everything[0:1, :], (T, T)).T
    factor = lax.rsqrt(everything / (HW * TP) + EPSILON)
    for j in range(0, HW, 128):
        mixer_ref[:, j : j + 128] = (
            gated[:, j : j + 128] * factor * gain_ref[:, j : j + 128]
        ).astype(BF16)

    def results_arrive(j):
        arrived(o_in.at[j], pair_send.at[3, 0], pair_recv.at[3, j], across)
        attn_ref[:, q_columns(j)] = o_in[j]

    pl.when(~own_slot)(lambda: results_arrive(x))
    results_arrive(1 - x)
    for pieces in [*quad, *returned, totals_sent]:
        for condition, copy in pieces:
            pl.when(condition)(copy.wait_send)
    for copy in sent:
        copy.wait_send()


def shards(dims, *args):
    (x, gate, b, c, step, bias, rate, skip, wx, wb, wc, gain, q, k, v) = args
    bias, rate, skip, gain = (a.reshape(1, -1) for a in (bias, rate, skip, gain))
    Y, Z, TP = dims
    T, HW = x.shape
    W = HW // Z
    G = b.shape[1] // STATE
    count = 2 * Y * Z
    QW = q.shape[1] // 2
    rows = QW // HD * T
    vmem, dma = pltpu.VMEM, pltpu.SemaphoreType.DMA
    scratch = [
        *(vmem(a.shape, BF16) for a in (x, gate, b, c, q, k, v)),
        dma((7,)),
        vmem((TAIL, HW), BF16),
        vmem((TAIL, G * STATE), BF16),
        vmem((TAIL, G * STATE), BF16),
        vmem((T + 8, W), F32),
        vmem((T + 8, G * STATE), F32),
        vmem((T, G * STATE), F32),
        vmem((T, G * STATE), F32),
        vmem((T, HW), BF16),
        vmem((TAIL, HW), F32),
        vmem((TAIL, HW), F32),
        vmem((8, HW), F32),
        vmem((T, HW), F32),
        vmem((T, HW), BF16),
        vmem((T, HW), F32),
        vmem((8, HW), F32),
        vmem((G, STATE, T), BF16),
        vmem((G, T, STATE), BF16),
        vmem((G, T, STATE), BF16),
        vmem((T, STATE), F32),
        vmem((STATE, T), F32),
        vmem((2, Z, STATE, W // 2), BF16),
        vmem((Z, 8, 128), F32),
        vmem((2, Z, STATE, W // 2), BF16),
        vmem((Z, 8, 128), F32),
        vmem((2, Z, STATE, W // 2), F32),
        vmem((2, STATE, W // 2), BF16),
        vmem((8, 128), F32),
        vmem((2, 2 * Y, STATE, W // 2), BF16),
        vmem((2 * Y, 8, 128), F32),
        vmem((2, Z, STATE, W // 2), BF16),
        vmem((2, Z, STATE, W // 2), BF16),
        vmem((T, HW), F32),
        vmem((T, HW), F32),
        vmem((TP, 8, 128), F32),
        vmem((2, count * T, HD), BF16),
        vmem((2, T, QW), BF16),
        vmem((2, rows, HD), BF16),
        vmem((2, T, QW), BF16),
        vmem((2, T, QW), BF16),
        vmem((2, rows, HD), F32),
        vmem((2, rows, 2 * HD), F32),
        dma((3,)),
        dma((3,)),
        dma((4, 3)),
        dma((4, 2)),
        dma((2, 2, max(Z // 2, 1))),
        dma((2, 2, max(Z // 2, 1))),
        dma((2, 3, Z)),
        dma((2, 3, Z)),
        dma((3, Z)),
        dma((3, Z)),
        dma((3, 2 * Y)),
        dma((3, 2 * Y)),
        dma((2, Z)),
        dma((2, Z)),
        dma((TP,)),
        dma((TP,)),
    ]
    whole = pl.BlockSpec(memory_space=pltpu.VMEM)
    return pl.pallas_call(
        functools.partial(kernel, dims),
        out_shape=(
            jax.ShapeDtypeStruct((T, HW), BF16),
            jax.ShapeDtypeStruct((T, 2 * QW), BF16),
        ),
        in_specs=[
            pl.BlockSpec(memory_space=pl.ANY) if a.dtype == BF16 else whole for a in args
        ],
        out_specs=(whole, whole),
        scratch_shapes=scratch,
        compiler_params=pltpu.CompilerParams(
            collective_id=0, has_side_effects=True, vmem_limit_bytes=60 * 1024 * 1024
        ),
        name="hybrid",
    )(x, gate, b, c, step.T, bias, rate, skip, wx, wb, wc, gain, q, k, v)


def build(mesh, Y, Z):
    TP = mesh.shape["tp"]
    torus = Mesh(mesh.devices.reshape(2, Y, Z, TP), (*SEQ, "tp"))
    cut, by_tp = P(SEQ, "tp"), P("tp")
    taps = P(None, "tp")
    placed = (cut,) * 5 + (by_tp,) * 3 + (taps,) * 3 + (by_tp,) + (cut,) * 3
    return jax.shard_map(
        functools.partial(shards, (Y, Z, TP)),
        mesh=torus,
        in_specs=placed,
        out_specs=(cut, cut),
        check_vma=False,
    )


def solution(mesh):
    return build(mesh, 4, 8)
```

```python
import functools
import math

import jax
import jax.numpy as jnp
from jax import lax
from jax.experimental import pallas as pl
from jax.experimental.pallas import tpu as pltpu
from jax.sharding import Mesh
from jax.sharding import PartitionSpec as P

P_SIZE = 64
STATE = 128
HD = 128
CONV = 4
SEQ = ("seq_0", "seq_1", "seq_2")
MESH = pl.DeviceIdType.MESH
F32 = jnp.float32
BF16 = jnp.bfloat16
HIGHEST = lax.Precision.HIGHEST
EPSILON = 1e-05
LOWEST = -1e30
KEY_TILE = 512
ROWS = 256
TAIL = 16


def nt(a, b, precision=None):
    return lax.dot_general(
        a, b, (((1,), (1,)), ((), ())), preferred_element_type=F32, precision=precision
    )


def nn(a, b, precision=None):
    return lax.dot_general(
        a, b, (((1,), (0,)), ((), ())), preferred_element_type=F32, precision=precision
    )


def silu(a):
    return a / (1.0 + jnp.exp(-a))


def two_parts(value):
    high = value.astype(BF16)
    low = (value - high.astype(F32)).astype(BF16)
    return high, low


def kernel(
    dims,
    x_far,
    gate_far,
    b_far,
    c_far,
    step_ref,
    bias_ref,
    rate_ref,
    skip_ref,
    wx_ref,
    wb_ref,
    wc_ref,
    gain_ref,
    q_far_in,
    k_far,
    v_far,
    mixer_ref,
    attn_ref,
    x_ref,
    gate_ref,
    b_ref,
    c_ref,
    q_ref,
    k_ref,
    v_ref,
    load_sems,
    tail_x,
    tail_b,
    tail_c,
    pad_x,
    pad_s,
    b_first,
    c_first,
    weighted,
    early_step,
    early_close,
    whole_decay,
    signal,
    scaled,
    entry_decay,
    skip_rows,
    b_turned,
    b_held,
    c_held,
    log_held,
    logt_held,
    state_out,
    decay_out,
    state_in,
    decay_in,
    prefix,
    total_out,
    total_decay_out,
    total_in,
    total_decay_in,
    enter_out,
    enter_in,
    diagonal,
    gated,
    squares,
    kv,
    q_far,
    q_rows,
    o_far,
    o_in,
    m_held,
    acc_held,
    tail_send,
    tail_recv,
    pair_send,
    pair_recv,
    ring_send,
    ring_recv,
    row_send,
    row_recv,
    a2a_send,
    a2a_recv,
    tot_send,
    tot_recv,
    back_send,
    back_recv,
    sq_send,
    sq_recv,
):
    Y, Z, TP = dims
    T = x_ref.shape[0]
    HW = x_ref.shape[1]
    heads = HW // P_SIZE
    W = HW // Z
    G = b_ref.shape[1] // STATE
    GW = HW // G
    YZ = Y * Z
    QW = q_ref.shape[1] // 2
    grouped = QW // HD

    x = lax.axis_index("seq_0")
    y = lax.axis_index("seq_1")
    z = lax.axis_index("seq_2")
    t = lax.axis_index("tp")
    seq = x * YZ + y * Z + z
    count = 2 * YZ

    def place(index):
        return (index // YZ, (index // Z) % Y, index % Z, t)

    after = place((seq + 1) % count)
    before = place((seq + count - 1) % count)

    core = t % 2
    high = y // (Y // 2)
    own_slot = (core + high) % 2 == 0
    facing = Y - 1 - y
    beside = y + 1 - 2 * (y % 2)
    sibling = (x, y, z, t + 1 - 2 * core)

    def z_peer(d):
        return (x, y, (z + d) % Z, t)

    y_peer = (x, beside, z, t)

    group = x * Y + y

    def group_peer(d):
        other = (group + d) % (2 * Y)
        return (other // Y, other % Y, z, t)

    def tp_peer(d):
        return (x, y, z, (t + d) % TP)

    total_in[...] = jnp.zeros(total_in.shape, BF16)
    total_decay_in[...] = jnp.ones(total_decay_in.shape, F32)
    barrier = pltpu.get_barrier_semaphore()
    greeted = [after, before]
    greeted += [z_peer(d) for d in range(1, Z)]
    greeted += [group_peer(d) for d in range(1, 2 * Y)]
    greeted += [tp_peer(d) for d in range(1, TP)]
    greeted += [(1 - x, y, z, t + 1 - 2 * core), (x, facing, z, t + 1 - 2 * core)]
    for peer in greeted:
        pl.semaphore_signal(barrier, inc=1, device_id=peer, device_id_type=MESH)

    def remote(src, dst, send, recv, peer):
        return pltpu.make_async_remote_copy(
            src_ref=src,
            dst_ref=dst,
            send_sem=send,
            recv_sem=recv,
            device_id=peer,
            device_id_type=MESH,
        )

    sent = []
    inside = jnp.where(seq > 0, 1.0, 0.0).astype(F32)
    far = (x_far, b_far, c_far, k_far, v_far, q_far_in, gate_far)
    held = (x_ref, b_ref, c_ref, k_ref, v_ref, q_ref, gate_ref)
    loads = [
        pltpu.make_async_copy(src, dst, load_sems.at[i]) for i, (src, dst) in enumerate(zip(far, held))
    ]
    for load in loads:
        load.start()

    def start(src, dst, send, recv, peer):
        copy = remote(src, dst, send, recv, peer)
        copy.start()
        sent.append(copy)

    def arrived(dst, send, recv, peer):
        remote(dst, dst, send, recv, peer).wait_recv()

    def block_of(slot, sharer, other, zz):
        xx = (x + core + sharer + high + slot) % 2
        low = facing * high + y * (1 - high)
        low = low * (1 - other) + (Y // 2 - 1 - low) * other
        up = (high + slot) % 2
        return xx * YZ + (low * (1 - up) + (Y - 1 - low) * up) * Z + zz

    def kv_at(slot, sharer, other, zz):
        first = pl.multiple_of(block_of(slot, sharer, other, zz) * T, T)
        return kv.at[:, pl.ds(first, T), :]

    own_rows = pl.ds(pl.multiple_of(seq * T, T), T)

    turned = jnp.concatenate(
        [step_ref[...], jnp.zeros((STATE - heads, T), F32)], axis=0
    ).T
    step_in = turned[:, :heads] + bias_ref[...]
    step = jnp.maximum(step_in, 0.0) + jnp.log(1.0 + jnp.exp(-jnp.abs(step_in)))
    rows_at = lax.broadcasted_iota(jnp.int32, (T, T), 0)
    cols_at = lax.broadcasted_iota(jnp.int32, (T, T), 1)
    lower = jnp.where(rows_at >= cols_at, 1.0, 0.0).astype(F32)
    wide = jnp.concatenate(
        [-step * rate_ref[...], jnp.zeros((T, STATE - heads), F32)], axis=1
    )
    log_decay = nn(lower, wide, HIGHEST)
    log_held[...] = log_decay
    logt_held[...] = log_decay.T
    log_decay = log_decay[:, :heads]
    last = log_decay[T - 1 : T, :]
    closing = jnp.exp(last - log_decay)
    columns = jnp.concatenate([step, step * closing, jnp.exp(log_decay)], axis=0)
    columns_high, columns_low = two_parts(columns)
    whole = jnp.concatenate(
        [
            jnp.broadcast_to(jnp.exp(last), (8, heads)),
            jnp.broadcast_to(skip_ref[...], (8, heads)),
        ],
        axis=0,
    )
    whole_high, whole_low = two_parts(whole)

    def conv_silu(pad, tail, rows, weights):
        count = rows.shape[0]
        if tail is None:
            pad[0:8, :] = jnp.zeros((8, rows.shape[1]), F32)
        else:
            pad[0:8, :] = tail[8:16, :].astype(F32) * inside
        pad[8 : count + 8, :] = rows.astype(F32)
        total = weights[0:1, :] * pad[5 : count + 5, :]
        for k in range(1, CONV):
            total = total + weights[k : k + 1, :] * pad[5 + k : count + 5 + k, :]
        return silu(total)

    for load in loads[:-1]:
        load.wait()

    @pl.when(own_slot)
    def _():
        kv[0, own_rows, :] = k_ref[:, pl.ds(pl.multiple_of(x * HD, HD), HD)]
        kv[1, own_rows, :] = v_ref[:, pl.ds(pl.multiple_of(x * HD, HD), HD)]
        for h in range(grouped):
            q_rows[0, h * T : (h + 1) * T, :] = q_ref[
                :, pl.ds(pl.multiple_of(x * QW + h * HD, HD), HD)
            ]

    pl.semaphore_wait(barrier, len(greeted))

    start(x_ref.at[T - TAIL :, :], tail_x, tail_send.at[0], tail_recv.at[0], after)
    start(b_ref.at[T - TAIL :, :], tail_b, tail_send.at[1], tail_recv.at[1], after)
    start(c_ref.at[T - TAIL :, :], tail_c, tail_send.at[2], tail_recv.at[2], after)
    across = (1 - x, y, z, t + 1 - 2 * core)
    face = (x, facing, z, t + 1 - 2 * core)
    corner = (1 - x, facing, z, t)

    def kv_columns(j):
        return pl.ds(pl.multiple_of(j * HD, HD), HD)

    def q_columns(j):
        return pl.ds(pl.multiple_of(j * QW, QW), QW)

    def pair_copies(what):
        found = []
        for condition, j, slot, peer in (
            (own_slot, 1 - x, 0, across),
            (~own_slot, x, 1, face),
            (~own_slot, 1 - x, 1, corner),
        ):
            n = len(found)
            if what == 2:
                copy = remote(
                    q_ref.at[:, q_columns(j)], q_far.at[slot], pair_send.at[2, n],
                    pair_recv.at[2, slot], peer,
                )
            else:
                copy = remote(
                    (k_ref, v_ref)[what].at[:, kv_columns(j)], kv.at[what, own_rows, :],
                    pair_send.at[what, n], pair_recv.at[what, slot], peer,
                )
            found.append((condition, copy))
        return found

    def back_copies():
        found = []
        for condition, slot, peer in (
            (~own_slot, 0, across),
            (~own_slot, 1, face),
            (own_slot, 1, corner),
        ):
            found.append(
                (
                    condition,
                    remote(
                        o_far.at[slot], o_in.at[x], pair_send.at[3, len(found)],
                        pair_recv.at[3, x], peer,
                    ),
                )
            )
        return found

    def start_all(pieces):
        for condition, copy in pieces:
            pl.when(condition)(copy.start)

    quad = [pair_copies(0), pair_copies(1)]
    for pieces in quad:
        start_all(pieces)

    right_steps = Z // 2
    left_steps = (Z - 1) // 2

    def ring_start(slot, s):
        if s < right_steps:
            piece = kv_at(slot, 0, 0, (z + Z - s) % Z)
            start(piece, piece, ring_send.at[slot, 0, s], ring_recv.at[slot, 0, s], z_peer(1))
        if s < left_steps:
            piece = kv_at(slot, 0, 0, (z + s) % Z)
            start(piece, piece, ring_send.at[slot, 1, s], ring_recv.at[slot, 1, s], z_peer(Z - 1))

    def ring_wait(slot, s):
        if s < right_steps:
            piece = kv_at(slot, 0, 0, (z + Z - 1 - s) % Z)
            arrived(piece, ring_send.at[slot, 0, s], ring_recv.at[slot, 0, s], z_peer(Z - 1))
        if s < left_steps:
            piece = kv_at(slot, 0, 0, (z + 1 + s) % Z)
            arrived(piece, ring_send.at[slot, 1, s], ring_recv.at[slot, 1, s], z_peer(1))

    def row_start(slot, d):
        piece = kv_at(slot, 0, 0, (z + d) % Z)
        start(piece, piece, row_send.at[slot, 0, d], row_recv.at[slot, 0, d], y_peer)
        start(piece, piece, row_send.at[slot, 1, d], row_recv.at[slot, 1, d], sibling)

    def near_arrives(slot, d):
        piece = kv_at(slot, 1, 0, (z + d) % Z)
        arrived(piece, row_send.at[slot, 1, d], row_recv.at[slot, 1, d], sibling)

    def row_forward(slot, d):
        piece = kv_at(slot, 0, 1, (z + d) % Z)
        arrived(piece, row_send.at[slot, 0, d], row_recv.at[slot, 0, d], y_peer)
        start(piece, piece, row_send.at[slot, 2, d], row_recv.at[slot, 2, d], sibling)

    def row_last(slot, d):
        piece = kv_at(slot, 1, 1, (z + d) % Z)
        arrived(piece, row_send.at[slot, 2, d], row_recv.at[slot, 2, d], sibling)

    def offsets(s):
        found = []
        if s < right_steps:
            found.append(Z - 1 - s)
        if s < left_steps:
            found.append(1 + s)
        return found

    quad.append(pair_copies(2))
    start_all(quad[2])

    def pair_arrives(slot):
        def wait():
            for i in range(2):
                place = block_of(slot, 0, 0, z)
                arrived(
                    kv.at[i, pl.ds(pl.multiple_of(place * T, T), T), :],
                    pair_send.at[i, 0],
                    pair_recv.at[i, slot],
                    across,
                )

        if slot == 0:
            pl.when(~own_slot)(wait)
        else:
            wait()
        ring_start(slot, 0)
        row_start(slot, 0)

    b_first[...] = conv_silu(pad_s, None, b_ref[...], wb_ref)
    c_first[...] = conv_silu(pad_s, None, c_ref[...], wc_ref)
    for k in range(Z):
        at = slice(k * W, (k + 1) * W)
        spread = jnp.where(
            lax.broadcasted_iota(jnp.int32, (heads, W), 0)
            == k * (W // P_SIZE) + lax.broadcasted_iota(jnp.int32, (heads, W), 1) // P_SIZE,
            1.0,
            0.0,
        ).astype(BF16)
        per_lane = nn(columns_high, spread) + nn(columns_low, spread)
        per_whole = nn(whole_high, spread) + nn(whole_low, spread)
        now = conv_silu(pad_x, None, x_ref[:, at], wx_ref[:, at])
        signal[:, at] = now
        scaled[:, at] = (now * per_lane[:T]).astype(BF16)
        weighted[:, at] = (now * per_lane[T : 2 * T]).astype(BF16)
        early_step[:, at] = per_lane[:TAIL]
        early_close[:, at] = per_lane[T : T + TAIL]
        entry_decay[:, at] = per_lane[2 * T :]
        skip_rows[:, at] = per_whole[8:]
        whole_decay[:, at] = per_whole[:8]


    HALF = W // 2
    chunks = W // 128

    def pack(row):
        parts = [row[:, i * 128 : (i + 1) * 128] for i in range(chunks)]
        if chunks < 8:
            parts.append(jnp.ones((8 - chunks, 128), F32))
        return jnp.concatenate(parts, axis=0)

    for d in [*range(1, Z), 0]:
        at = pl.ds(pl.multiple_of((z + d) % Z * W, W), W)
        packed = pack(whole_decay[0:1, at])
        if d:
            decay_out[d] = packed
            start(decay_out.at[d], decay_in.at[z], a2a_send.at[2, d], a2a_recv.at[2, d], z_peer(d))
        else:
            decay_in[z] = packed

    arrived(tail_x, tail_send.at[0], tail_recv.at[0], before)
    arrived(tail_b, tail_send.at[1], tail_recv.at[1], before)
    arrived(tail_c, tail_send.at[2], tail_recv.at[2], before)
    b_first[:TAIL, :] = conv_silu(pad_s, tail_b, b_ref[:TAIL, :], wb_ref)
    c_first[:TAIL, :] = conv_silu(pad_s, tail_c, c_ref[:TAIL, :], wc_ref)
    for g in range(G):
        cols = slice(g * STATE, (g + 1) * STATE)
        b_held[g] = b_first[:, cols].astype(BF16)
        b_turned[g] = b_first[:, cols].T.astype(BF16)
        c_held[g] = c_first[:, cols].astype(BF16)
    for k in range(Z):
        at = slice(k * W, (k + 1) * W)
        now = conv_silu(pad_x, tail_x[:, at], x_ref[:TAIL, at], wx_ref[:, at])
        signal[:TAIL, at] = now
        scaled[:TAIL, at] = (now * early_step[:, at]).astype(BF16)
        weighted[:TAIL, at] = (now * early_close[:, at]).astype(BF16)
    pair_arrives(0)
    pair_arrives(1)

    def unpack(packed, half):
        return jnp.concatenate(
            [packed[i : i + 1] for i in range(half * chunks // 2, (half + 1) * chunks // 2)], axis=1
        )

    def advance(half, s):
        if s < right_steps:
            ring_wait(half, s)
            if s + 1 < right_steps:
                ring_start(half, s + 1)
            for d in offsets(s):
                row_start(half, d)

    def slice_of_heads(d):
        k = (z + d) % Z
        at = pl.ds(pl.multiple_of(k * W, W), W)
        state = nn(b_turned[k * W // GW], weighted[:, at]).astype(BF16)
        if d:
            for half in range(2):
                state_out[half, d] = state[:, half * HALF : (half + 1) * HALF]
        else:
            for half in range(2):
                state_in[half, z] = state[:, half * HALF : (half + 1) * HALF]

    def start_state(half, d):
        start(
            state_out.at[half, d],
            state_in.at[half, z],
            a2a_send.at[half, d],
            a2a_recv.at[half, d],
            z_peer(d),
        )

    for d in [*range(1, Z), 0]:
        slice_of_heads(d)

    causal = rows_at >= cols_at
    couplings = [nt(c_held[g], b_held[g]) for g in range(G)]
    lane_at = lax.broadcasted_iota(jnp.int32, (T, 2 * P_SIZE), 1)

    def pair_of_heads(p):
        mixes = []
        for h in (2 * p, 2 * p + 1):
            spread = log_held[:, h : h + 1] - logt_held[h : h + 1, :]
            decays = jnp.exp(jnp.where(causal, spread, LOWEST))
            mixes.append((decays * couplings[h * P_SIZE // GW]).astype(BF16))
        two = scaled[:, p * 128 : (p + 1) * 128]
        zero = jnp.zeros_like(two)
        stacked = jnp.concatenate(
            [jnp.where(lane_at < P_SIZE, two, zero), jnp.where(lane_at < P_SIZE, zero, two)],
            axis=0,
        )
        diagonal[:, p * 128 : (p + 1) * 128] = nn(jnp.concatenate(mixes, axis=1), stacked)

    pairs = heads // 2

    def some_pairs(low, high):
        for p in range(low * pairs // 16, high * pairs // 16):
            pair_of_heads(p)

    def ring_step(s):
        for slot in range(2):
            advance(slot, s)

    for d in range(1, Z):
        source = (z + Z - d) % Z
        arrived(decay_in.at[source], a2a_send.at[2, d], a2a_recv.at[2, d], z_peer(Z - d))
    running_decay = jnp.ones((8, 128), F32)
    for i in range(Z):
        running_decay = running_decay * decay_in[i]
    total_decay_out[...] = running_decay
    total_decay_in[group] = running_decay
    totals_sent = []

    def total_start(src, dst, kind, d):
        copy = remote(src, dst, tot_send.at[kind, d], tot_recv.at[kind, d], group_peer(d))
        later = group + d < 2 * Y
        pl.when(later)(copy.start)
        totals_sent.append((later, copy))

    def total_arrived(dst, kind, d):
        @pl.when(group >= d)
        def _():
            arrived(dst, tot_send.at[kind, d], tot_recv.at[kind, d], group_peer(2 * Y - d))

    for d in range(1, 2 * Y):
        total_start(total_decay_out, total_decay_in.at[group], 2, d)

    def scan(half):
        for d in range(1, Z):
            source = (z + Z - d) % Z
            arrived(
                state_in.at[half, source], a2a_send.at[half, d], a2a_recv.at[half, d], z_peer(Z - d)
            )
        running = jnp.zeros((STATE, HALF), F32)
        for i in range(Z):
            prefix[half, i] = running
            running = running * unpack(decay_in[i], half) + state_in[half, i].astype(F32)
        total_out[half] = running.astype(BF16)
        total_in[half, group] = running.astype(BF16)
        for d in range(1, 2 * Y):
            total_start(total_out.at[half], total_in.at[half, group], half, d)

    def enter(half):
        for d in range(1, 2 * Y):
            source = (group + 2 * Y - d) % (2 * Y)
            if half == 0:
                total_arrived(total_decay_in.at[source], 2, d)
            total_arrived(total_in.at[half, source], half, d)
        entering = jnp.zeros((STATE, HALF), F32)
        for i in range(2 * Y):
            further = entering * unpack(total_decay_in[i], half) + total_in[half, i].astype(F32)
            entering = jnp.where(i < group, further, entering)
        so_far = jnp.ones((8, 128), F32)
        for i in range(Z):
            enter_out[half, i] = (prefix[half, i] + entering * unpack(so_far, half)).astype(BF16)
            so_far = so_far * decay_in[i]
        for d in range(1, Z):
            k = (z + d) % Z
            start(
                enter_out.at[half, k],
                enter_in.at[half, z],
                back_send.at[half, d],
                back_recv.at[half, d],
                z_peer(d),
            )
        enter_in[half, z] = enter_out[half, z]

    piece_order = [0]
    for n in range(right_steps):
        piece_order += offsets(n)
    scale = math.log2(math.e) / math.sqrt(HD)
    all_rows = grouped * T
    chunk = min(ROWS, all_rows)

    span = max(Z // 2, 1)
    key_tile = span * T
    m_held[...] = jnp.full(m_held.shape, LOWEST, F32)
    acc_held[...] = jnp.zeros(acc_held.shape, F32)

    def tile(which, start_key, position, masked):
        keys_at = pl.ds(pl.multiple_of(start_key, key_tile), key_tile)
        keys = kv[0, keys_at, :]
        values = jnp.concatenate([kv[1, keys_at, :], jnp.ones((key_tile, HD), BF16)], axis=1)
        for r in range(0, all_rows, chunk):
            scores = nt(q_rows[which, r : r + chunk, :], keys)
            if masked:
                row = lax.broadcasted_iota(jnp.int32, (chunk, key_tile), 0) % T
                col = lax.broadcasted_iota(jnp.int32, (chunk, key_tile), 1)
                scores = jnp.where(col + start_key <= row + position * T, scores, LOWEST)
            old = m_held[which, r : r + chunk, :]
            new = jnp.maximum(old, jnp.max(scores, axis=1, keepdims=True))
            m_held[which, r : r + chunk, :] = new
            factor = jnp.exp2((old - new) * scale)
            weights = jnp.concatenate(
                [
                    jnp.exp2((scores[:, j : j + HD] - new) * scale).astype(BF16)
                    for j in range(0, key_tile, HD)
                ],
                axis=1,
            )
            product = nn(weights, values)
            acc_held[which, r : r + chunk, :] = (
                acc_held[which, r : r + chunk, :] * jnp.concatenate([factor, factor], axis=1)
                + product
            )

    def attend(other, which, parts):
        near = z // span

        def one(i, carry):
            n = (near + parts[0] + i // 4) % 2
            sharer, slot = i // 2 % 2, i % 2
            position = block_of(which, 0, 0, z)
            first = block_of(slot, sharer, other, 0) + n * span

            @pl.when(first + span <= position)
            def _():
                tile(which, first * T, position, False)

            @pl.when((first <= position) & (position < first + span))
            def _():
                tile(which, first * T, position, True)

            return carry

        lax.fori_loop(0, 4 * len(parts), one, 0)

    def unroll_queries(slot):
        arrived(q_far.at[slot], pair_send.at[2, 0], pair_recv.at[2, slot], across)
        for h in range(grouped):
            q_rows[slot, h * T : (h + 1) * T, :] = q_far[slot, :, h * HD : (h + 1) * HD]

    def result(which, h):
        both = acc_held[which, h * T : (h + 1) * T, :]
        return (both[:, :HD] / both[:, HD:]).astype(BF16)

    def results_leave(slot):
        for h in range(grouped):
            o_far[slot, :, h * HD : (h + 1) * HD] = result(slot, h)
        start_all(returned[slot])

    returned = back_copies()
    returned = [returned[:1], returned[1:]]

    def forward(pieces):
        for d in pieces:
            for slot in range(2):
                row_forward(slot, d)

    far_first = sorted(range(1, Z), key=lambda d: -min(d, Z - d))
    first, second = far_first[: Z // 2], far_first[Z // 2 :]

    def states(half, which):
        for d in which:
            start_state(half, d)

    def near(pieces):
        for d in pieces:
            for slot in range(2):
                near_arrives(slot, d)

    some_pairs(0, 8)
    ring_step(0)
    states(0, first)
    ring_step(1)
    states(0, second)
    ring_step(2)
    some_pairs(8, 16)
    states(1, first)
    states(1, second)
    pl.when(~own_slot)(lambda: unroll_queries(0))
    unroll_queries(1)
    near([d for d in piece_order if d != Z // 2])
    attend(0, 1, (0,))
    ring_step(3)
    near([Z // 2])
    attend(0, 0, (0,))
    scan(0)
    attend(0, 1, (1,))
    scan(1)
    attend(0, 0, (1,))
    enter(0)
    forward(piece_order)
    for d in piece_order:
        for slot in range(2):
            row_last(slot, d)
    enter(1)
    attend(1, 1, (0, 1))
    results_leave(1)
    attend(1, 0, (0, 1))
    results_leave(0)

    @pl.when(own_slot)
    def _():
        attn_ref[:, q_columns(x)] = o_far[0]

    for d in range(1, Z):
        source = (z + Z - d) % Z
        for half in range(2):
            arrived(
                enter_in.at[half, source], back_send.at[half, d], back_recv.at[half, d], z_peer(Z - d)
            )
    loads[-1].wait()
    summed = jnp.zeros((T, 128), F32)
    for k in range(Z):
        cols = slice(k * W, (k + 1) * W)
        entry = jnp.concatenate([enter_in[0, k], enter_in[1, k]], axis=1)
        off = nn(c_held[k * W // GW], entry)
        mixed = diagonal[:, cols] + entry_decay[:, cols] * off
        mixed = mixed + skip_rows[0:1, cols] * signal[:, cols]
        now = mixed * silu(gate_ref[:, cols].astype(F32))
        gated[:, cols] = now
        now = now * now
        for j in range(0, W, 128):
            summed = summed + now[:, j : j + 128]
    squares[t] = nt(jnp.ones((8, 128), F32), summed, HIGHEST)
    for d in range(1, TP):
        start(squares.at[t], squares.at[t], sq_send.at[d], sq_recv.at[d], tp_peer(d))
    for d in range(1, TP):
        source = (t + TP - d) % TP
        arrived(squares.at[source], sq_send.at[d], sq_recv.at[d], tp_peer(TP - d))
    everything = squares[0]
    for i in range(1, TP):
        everything = everything + squares[i]
    everything = jnp.broadcast_to(everything[0:1, :], (T, T)).T
    factor = lax.rsqrt(everything / (HW * TP) + EPSILON)
    for j in range(0, HW, 128):
        mixer_ref[:, j : j + 128] = (
            gated[:, j : j + 128] * factor * gain_ref[:, j : j + 128]
        ).astype(BF16)

    def results_arrive(j):
        arrived(o_in.at[j], pair_send.at[3, 0], pair_recv.at[3, j], across)
        attn_ref[:, q_columns(j)] = o_in[j]

    pl.when(~own_slot)(lambda: results_arrive(x))
    results_arrive(1 - x)
    for pieces in [*quad, *returned, totals_sent]:
        for condition, copy in pieces:
            pl.when(condition)(copy.wait_send)
    for copy in sent:
        copy.wait_send()


def shards(dims, *args):
    (x, gate, b, c, step, bias, rate, skip, wx, wb, wc, gain, q, k, v) = args
    bias, rate, skip, gain = (a.reshape(1, -1) for a in (bias, rate, skip, gain))
    Y, Z, TP = dims
    T, HW = x.shape
    W = HW // Z
    G = b.shape[1] // STATE
    count = 2 * Y * Z
    QW = q.shape[1] // 2
    rows = QW // HD * T
    vmem, dma = pltpu.VMEM, pltpu.SemaphoreType.DMA
    scratch = [
        *(vmem(a.shape, BF16) for a in (x, gate, b, c, q, k, v)),
        dma((7,)),
        vmem((TAIL, HW), BF16),
        vmem((TAIL, G * STATE), BF16),
        vmem((TAIL, G * STATE), BF16),
        vmem((T + 8, W), F32),
        vmem((T + 8, G * STATE), F32),
        vmem((T, G * STATE), F32),
        vmem((T, G * STATE), F32),
        vmem((T, HW), BF16),
        vmem((TAIL, HW), F32),
        vmem((TAIL, HW), F32),
        vmem((8, HW), F32),
        vmem((T, HW), F32),
        vmem((T, HW), BF16),
        vmem((T, HW), F32),
        vmem((8, HW), F32),
        vmem((G, STATE, T), BF16),
        vmem((G, T, STATE), BF16),
        vmem((G, T, STATE), BF16),
        vmem((T, STATE), F32),
        vmem((STATE, T), F32),
        vmem((2, Z, STATE, W // 2), BF16),
        vmem((Z, 8, 128), F32),
        vmem((2, Z, STATE, W // 2), BF16),
        vmem((Z, 8, 128), F32),
        vmem((2, Z, STATE, W // 2), F32),
        vmem((2, STATE, W // 2), BF16),
        vmem((8, 128), F32),
        vmem((2, 2 * Y, STATE, W // 2), BF16),
        vmem((2 * Y, 8, 128), F32),
        vmem((2, Z, STATE, W // 2), BF16),
        vmem((2, Z, STATE, W // 2), BF16),
        vmem((T, HW), F32),
        vmem((T, HW), F32),
        vmem((TP, 8, 128), F32),
        vmem((2, count * T, HD), BF16),
        vmem((2, T, QW), BF16),
        vmem((2, rows, HD), BF16),
        vmem((2, T, QW), BF16),
        vmem((2, T, QW), BF16),
        vmem((2, rows, HD), F32),
        vmem((2, rows, 2 * HD), F32),
        dma((3,)),
        dma((3,)),
        dma((4, 3)),
        dma((4, 2)),
        dma((2, 2, max(Z // 2, 1))),
        dma((2, 2, max(Z // 2, 1))),
        dma((2, 3, Z)),
        dma((2, 3, Z)),
        dma((3, Z)),
        dma((3, Z)),
        dma((3, 2 * Y)),
        dma((3, 2 * Y)),
        dma((2, Z)),
        dma((2, Z)),
        dma((TP,)),
        dma((TP,)),
    ]
    whole = pl.BlockSpec(memory_space=pltpu.VMEM)
    return pl.pallas_call(
        functools.partial(kernel, dims),
        out_shape=(
            jax.ShapeDtypeStruct((T, HW), BF16),
            jax.ShapeDtypeStruct((T, 2 * QW), BF16),
        ),
        in_specs=[
            pl.BlockSpec(memory_space=pl.ANY) if a.dtype == BF16 else whole for a in args
        ],
        out_specs=(whole, whole),
        scratch_shapes=scratch,
        compiler_params=pltpu.CompilerParams(
            collective_id=0, has_side_effects=True, vmem_limit_bytes=60 * 1024 * 1024
        ),
        name="hybrid",
    )(x, gate, b, c, step.T, bias, rate, skip, wx, wb, wc, gain, q, k, v)


def build(mesh, Y, Z):
    TP = mesh.shape["tp"]
    torus = Mesh(mesh.devices.reshape(2, Y, Z, TP), (*SEQ, "tp"))
    cut, by_tp = P(SEQ, "tp"), P("tp")
    taps = P(None, "tp")
    placed = (cut,) * 5 + (by_tp,) * 3 + (taps,) * 3 + (by_tp,) + (cut,) * 3
    return jax.shard_map(
        functools.partial(shards, (Y, Z, TP)),
        mesh=torus,
        in_specs=placed,
        out_specs=(cut, cut),
        check_vma=False,
    )


def solution(mesh):
    return build(mesh, 4, 8)
```
